32 devices in a mesh: seq: 8 (over y, x, core), head: 4 (over z).
Axes of the slice: x: 2, y: 2, z: 4, core: 2. Of those that a mesh axis runs over, the one named last changes fastest.
Arguments:
- mid: bfloat16 [2048, 3072], P('seq'), may hold values from -20 to 20
- second_in: bfloat16 [2048, 3072], P('seq'), may hold values from -20 to 20
- cotangent: bfloat16 [2048, 3072], P('seq'), may hold values from -6 to 6
- w_key: bfloat16 [3072, 1024], P(None, 'head'), may hold values from -0.109375 to 0.109375
- w_value: bfloat16 [3072, 1024], P(None, 'head'), may hold values from -0.109375 to 0.109375
- w_query: bfloat16 [2, 3072, 3072], P(None, None, 'head'), may hold values from -0.109375 to 0.109375
- w_out: bfloat16 [2, 3072, 3072], P(None, 'head'), may hold values from -0.109375 to 0.109375
- w_ret_out: bfloat16 [3072, 3072], P('head'), may hold values from -0.109375 to 0.109375
- ret_query: bfloat16 [2048, 3072], P('seq', 'head'), may hold values from -6 to 6
- ret_key: bfloat16 [2048, 3072], P('seq', 'head'), may hold values from -3 to 3
- ret_value: bfloat16 [2048, 3072], P('seq', 'head'), may hold values from -6 to 6
- gate: float32 [24, 2048], P('head', 'seq'), may hold values from 0 to 6
- decay_exp: int32 [24], P('head'), may hold values from 0 to 256
- mask_start: int32 [16], P('seq'), may hold values from 0 to 1920, as said below
Outputs:
- grad_mid: bfloat16 [2048, 3072], P('seq')
- grad_ret_query: bfloat16 [2048, 3072], P('seq', 'head')
- grad_ret_key: bfloat16 [2048, 3072], P('seq', 'head')
- grad_ret_value: bfloat16 [2048, 3072], P('seq', 'head')
- grad_w_key: float32 [3072, 1024], P(None, 'head')
- grad_w_value: float32 [3072, 1024], P(None, 'head')
The draws below stay inside these ranges and needn't reach their ends.
Inputs may be any that keep to these rules, and one draw needn't show every extreme that they name: `mask_start`: the entry of each block of 128 queries is at most the position of that block's first query.
All inputs are finite; a program needn't handle non-finite values.
Results may differ from the reference program's by a relative error of at most 0.025.
The reference program's roundings to bfloat16 on the way count: a program that leaves them out, or rounds other values in their place, can miss the bound.
Values may be sent and summed in bfloat16 or wider, within the bound.
A program may use at most 192 MiB of HBM per device.

```python
import math
import jax
import jax.numpy as jnp
from jax import lax

D = 3072
H = 24
KVH = 8
HR = 24
E = 128
LAYERS = 2
BLK = 128
RC = 128
TOK_DEV = 256
TOKENS = 2048


def rows_with_peaks(key):
    values = jnp.clip(jax.random.normal(key, (TOKENS, D), jnp.float32), -5.0, 5.0)
    return values.astype(jnp.bfloat16)


def draw_mid(key, part):
    return rows_with_peaks(key)


def draw_second_in(key, part):
    return rows_with_peaks(jax.random.fold_in(key, 11))


def draw_gate(key, part):
    chooser, rough_key, block_key = jax.random.split(key, 3)
    portion = 0.5
    lasting = jax.random.uniform(chooser, (HR, 1), jnp.float32) < portion
    rough = jax.random.uniform(rough_key, (HR, TOKENS), jnp.float32, 0.5, 2.0)
    blocks = jax.random.uniform(block_key, (HR, TOKENS // TOK_DEV), jnp.float32, 0.5, 2.0)
    rough = rough * jnp.repeat(blocks, TOK_DEV, axis=1)
    factor = jnp.where(lasting, 0.5 / TOKENS, 1.5)
    return (factor * rough).astype(jnp.float32)


def draw_mask_start(key, part):
    blocks = TOKENS // BLK
    firsts = jnp.arange(blocks, dtype=jnp.int32) * BLK
    drawn = jax.random.randint(key, (blocks,), 0, firsts + 1, dtype=jnp.int32)
    last_block = jnp.arange(blocks, dtype=jnp.int32) == blocks - 1
    return jnp.where(last_block, firsts, drawn).astype(jnp.int32)


def with_ends(result, stream_key, least, top_value):
    longest = result.shape.index(max(result.shape))
    spots = []
    for shift in (0, 1):
        where = [jax.random.randint(jax.random.fold_in(stream_key, axis), (), 0, length) for axis, length in enumerate(result.shape)]
        where[longest] = (where[longest] + shift) % result.shape[longest]
        spots.append(tuple(where))
    return result.at[spots[0]].set(least).at[spots[1]].set(top_value)


def steps_of(rng, dims, cuts, smallest, high):
    loudness = 1.0
    for position, parts in cuts:
        steps = jax.random.uniform(jax.random.fold_in(jax.random.fold_in(rng, 6), position), (parts,), jnp.float32, smallest / len(cuts), high / len(cuts))
        loudness = loudness * jnp.repeat(jnp.exp(steps), dims[position] // parts).reshape((-1,) + (1,) * (len(dims) - 1 - position))
    return loudness


def gaussian(rng, shape, spread, bound, shards=(), kind=jnp.bfloat16):
    factor_of = steps_of(rng, shape, shards, -0.22, 0.18) if shards else 1.0
    result = jax.random.normal(rng, shape, jnp.float32) * spread * factor_of
    return jnp.minimum(jnp.maximum(result, -bound), bound).astype(kind)


def setup_inputs(seed: int = 0) -> dict:
    streams_of = jax.random.split(jax.random.key(seed), 15)
    return {
        "mid": draw_mid(jax.random.fold_in(streams_of[14], 71), 0),
        "second_in": draw_second_in(jax.random.fold_in(streams_of[14], 71), 0),
        "cotangent": gaussian(streams_of[2], (TOKENS, D), 1.0, 6.0, ((0, 8),)),
        "w_key": gaussian(streams_of[3], (D, KVH * E), D ** -0.5, 0.109375, ((1, 4),)),
        "w_value": gaussian(streams_of[4], (D, KVH * E), D ** -0.5, 0.109375, ((1, 4),)),
        "w_query": gaussian(streams_of[5], (LAYERS, D, H * E), D ** -0.5, 0.109375, ((2, 4),)),
        "w_out": gaussian(streams_of[6], (LAYERS, H * E, D), (H * E) ** -0.5, 0.109375, ((1, 4),)),
        "w_ret_out": gaussian(streams_of[7], (HR * E, D), (HR * E) ** -0.5, 0.109375, ((0, 4),)),
        "ret_query": gaussian(streams_of[8], (TOKENS, HR * E), 1.0, 6.0, ((0, 8), (1, 4))),
        "ret_key": gaussian(streams_of[9], (TOKENS, HR * E), 0.5, 3.0, ((0, 8), (1, 4))),
        "ret_value": gaussian(streams_of[10], (TOKENS, HR * E), 1.0, 6.0, ((0, 8), (1, 4))),
        "gate": draw_gate(jax.random.fold_in(streams_of[14], 71), 0),
        "decay_exp": with_ends(jax.random.randint(streams_of[12], (HR,), 0, 257), jax.random.fold_in(streams_of[12], 1), 0, 256).astype(jnp.int32),
        "mask_start": draw_mask_start(jax.random.fold_in(streams_of[14], 71), 0),
    }


def contract_last(left, right):
    return lax.dot_general(left, right, (((1,), (1,)), ((), ())), preferred_element_type=jnp.float32)

def round_trip(value):
    return lax.optimization_barrier(value.astype(jnp.bfloat16)).astype(jnp.float32)

def attend_back(layer_in, w_query_l, w_out_l, upstream, keys, values, visible):
    length = layer_in.shape[0]
    kv_heads = keys.shape[1] // E
    factor = 1.0 / math.sqrt(E)
    queries = jnp.dot(layer_in, w_query_l, preferred_element_type=jnp.float32).astype(jnp.bfloat16)
    group = queries.shape[1] // keys.shape[1]
    grad_out = contract_last(upstream, w_out_l).astype(jnp.bfloat16)
    query_heads = queries.reshape(length, kv_heads, group, E).transpose(1, 2, 0, 3)
    grad_heads = grad_out.reshape(length, kv_heads, group, E).transpose(1, 2, 0, 3)
    key_heads = keys.reshape(length, kv_heads, E).transpose(1, 0, 2)
    value_heads = values.reshape(length, kv_heads, E).transpose(1, 0, 2)

    def one_group(items):
        query_now = items[0].astype(jnp.float32)
        grad_now = items[1].astype(jnp.float32)
        key_now = items[2].astype(jnp.float32)
        value_now = items[3].astype(jnp.float32)
        scores = jnp.einsum('gte,se->gts', query_now, key_now) * factor
        scores = jnp.where(visible, scores, -jnp.inf)
        top = lax.optimization_barrier(jnp.max(scores, axis=-1, keepdims=True))
        raised = jnp.exp(scores - top)
        probs = raised / lax.optimization_barrier(jnp.sum(raised, axis=-1, keepdims=True))
        rounded = round_trip(probs)
        outputs = round_trip(jnp.einsum('gts,se->gte', rounded, value_now))
        delta = lax.optimization_barrier(jnp.sum(grad_now * outputs, axis=-1, keepdims=True))
        dprobs = jnp.einsum('gte,se->gts', grad_now, value_now)
        dscores = round_trip(probs * (dprobs - delta) * factor)
        query_grad = jnp.einsum('gts,se->gte', dscores, key_now).astype(jnp.bfloat16)
        key_part = jnp.einsum('gts,gte->se', dscores, query_now)
        value_part = jnp.einsum('gts,gte->se', rounded, grad_now)
        return (query_grad, key_part, value_part)
    query_grads, key_parts, value_parts = lax.map(one_group, (query_heads, grad_heads, key_heads, value_heads))
    query_grad = query_grads.transpose(2, 0, 1, 3).reshape(length, -1)
    key_part = key_parts.transpose(1, 0, 2).reshape(length, -1)
    value_part = value_parts.transpose(1, 0, 2).reshape(length, -1)
    return (contract_last(query_grad, w_query_l), key_part, value_part)

def retention_states(ret_key, ret_value, gate, decay_exp):
    length, width = ret_key.shape
    heads = gate.shape[0]
    size = width // heads
    count = length // RC
    key_blocks = ret_key.reshape(count, RC, heads, size).astype(jnp.float32)
    value_blocks = ret_value.reshape(count, RC, heads, size).astype(jnp.float32)
    rate = jnp.exp2(-decay_exp.astype(jnp.float32) / 64.0)
    accum = jnp.cumsum((-rate[:, None] * gate).reshape(heads, count, RC), axis=2)
    ends = accum[:, :, -1]
    shrink = jnp.transpose(jnp.exp(ends[:, :, None] - accum), (1, 2, 0))[..., None]
    own_state = jnp.einsum('csha,cshb->hcab', round_trip(shrink * key_blocks), value_blocks)
    return (accum, ends, shrink, own_state)

def grad_states(ret_query, grad_o, accum):
    heads, count, block = accum.shape
    size = ret_query.shape[1] // heads
    query_blocks = ret_query.reshape(count, block, heads, size).astype(jnp.float32)
    grad_blocks = grad_o.reshape(count, block, heads, size).astype(jnp.float32)
    grow = jnp.transpose(jnp.exp(accum), (1, 2, 0))[..., None]
    own_grad = jnp.einsum('ctha,cthb->hcab', round_trip(grow * query_blocks), grad_blocks) / E
    return (grow, own_grad)

def retention_grads(ret_query, ret_key, ret_value, grad_o, accum, shrink, grow, entering, after):
    length, width = ret_query.shape
    heads, count, block = accum.shape
    size = width // heads
    shape4 = (count, block, heads, size)
    query_blocks = ret_query.reshape(shape4).astype(jnp.float32)
    key_blocks = ret_key.reshape(shape4).astype(jnp.float32)
    value_blocks = ret_value.reshape(shape4).astype(jnp.float32)
    grad_blocks = grad_o.reshape(shape4).astype(jnp.float32)
    lower = jnp.arange(block)[:, None] >= jnp.arange(block)[None, :]
    diff = accum[:, :, :, None] - accum[:, :, None, :]
    weights = jnp.where(lower, jnp.exp(jnp.where(lower, diff, 0.0)), 0.0)
    first = round_trip(weights * jnp.einsum('ctha,csha->hcts', grad_blocks, value_blocks))
    second = round_trip(weights * jnp.einsum('ctha,csha->hcts', query_blocks, key_blocks))
    inner_query = jnp.einsum('hcts,csha->ctha', first, key_blocks)
    inner_key = jnp.einsum('hcts,ctha->csha', first, query_blocks)
    inner_value = jnp.einsum('hcts,ctha->csha', second, grad_blocks)
    highest = lax.Precision.HIGHEST
    carried_query = jnp.einsum('cthb,hcab->ctha', grad_blocks, entering, precision=highest)
    carried_key = jnp.einsum('cshb,hcab->csha', value_blocks, after, precision=highest)
    carried_value = jnp.einsum('csha,hcab->cshb', key_blocks, after, precision=highest)
    grad_query = ((inner_query + grow * carried_query) / E).astype(jnp.bfloat16).reshape(length, width)
    grad_key = (inner_key / E + shrink * carried_key).astype(jnp.bfloat16).reshape(length, width)
    grad_value = (inner_value / E + shrink * carried_value).astype(jnp.bfloat16).reshape(length, width)
    return (grad_query, grad_key, grad_value)

def reference(mid, second_in, cotangent, w_key, w_value, w_query, w_out, w_ret_out, ret_query, ret_key, ret_value, gate, decay_exp, mask_start):
    keys = jnp.dot(mid, w_key, preferred_element_type=jnp.float32).astype(jnp.bfloat16)
    values = jnp.dot(mid, w_value, preferred_element_type=jnp.float32).astype(jnp.bfloat16)
    positions = jnp.arange(TOKENS, dtype=jnp.int32)
    first_seen = jnp.repeat(mask_start, BLK)
    visible = (positions[None, :] >= first_seen[:, None]) & (positions[None, :] <= positions[:, None])
    upper_in, upper_key, upper_value = attend_back(second_in, w_query[1], w_out[1], cotangent, keys, values, visible)
    upstream = (cotangent.astype(jnp.float32) + upper_in).astype(jnp.bfloat16)
    lower_in, lower_key, lower_value = attend_back(mid, w_query[0], w_out[0], upstream, keys, values, visible)
    key_grad = (upper_key + lower_key).astype(jnp.bfloat16)
    value_grad = (upper_value + lower_value).astype(jnp.bfloat16)
    grad_mid = (upstream.astype(jnp.float32) + lower_in + contract_last(key_grad, w_key) + contract_last(value_grad, w_value)).astype(jnp.bfloat16)
    tokens_dims = (((0,), (0,)), ((), ()))
    grad_w_key = lax.dot_general(mid, key_grad, tokens_dims, preferred_element_type=jnp.float32)
    grad_w_value = lax.dot_general(mid, value_grad, tokens_dims, preferred_element_type=jnp.float32)
    grad_o = contract_last(grad_mid, w_ret_out).astype(jnp.bfloat16)
    accum, ends, shrink, own_state = retention_states(ret_key, ret_value, gate, decay_exp)
    grow, own_grad = grad_states(ret_query, grad_o, accum)
    decays = jnp.exp(ends)
    zeros = jnp.zeros((gate.shape[0], E, E), jnp.float32)

    def forward(state, items):
        return (items[0][:, None, None] * state + items[1], state)

    def backward(state, items):
        return (items[1] + items[0][:, None, None] * state, state)
    unused_state, entering = lax.scan(forward, zeros, (decays.T, jnp.moveaxis(own_state, 1, 0)))
    unused_grad, after = lax.scan(backward, zeros, (decays.T, jnp.moveaxis(own_grad, 1, 0)), reverse=True)
    entering = jnp.moveaxis(entering, 0, 1)
    after = jnp.moveaxis(after, 0, 1)
    grad_query, grad_key, grad_value = retention_grads(ret_query, ret_key, ret_value, grad_o, accum, shrink, grow, entering, after)
    return (grad_mid, grad_query, grad_key, grad_value, grad_w_key, grad_w_value)
```

```python
import functools
import math

import jax
import jax.numpy as jnp
from jax import lax
from jax.experimental import pallas as pl
from jax.experimental.pallas import tpu as pltpu
from jax.sharding import PartitionSpec as P

E = 128
BLK = 128
RC = 128
F32 = jnp.float32
BF16 = jnp.bfloat16


def contract_last(left, right):
    return lax.dot_general(left, right, (((1,), (1,)), ((), ())), preferred_element_type=F32)


def contract_first(left, right):
    return lax.dot_general(left, right, (((0,), (0,)), ((), ())), preferred_element_type=F32)


def send(src, dst, send_sem, recv_sem, axis, index):
    return pltpu.make_async_remote_copy(
        src_ref=src,
        dst_ref=dst,
        send_sem=send_sem,
        recv_sem=recv_sem,
        device_id={axis: index},
        device_id_type=pl.DeviceIdType.MESH,
    )


class SeqPlace:
    def __init__(self):
        self.peers = lax.axis_size("seq")
        self.chips = self.peers // 2
        self.me = lax.axis_index("seq")
        self.chip = self.me // 2
        self.core = lax.rem(self.me, 2)
        self.sibling = self.me + 1 - 2 * self.core

    def mate(self, k):
        return lax.rem(self.me + 2 * k, self.peers)

    def mate_of_sibling(self, k):
        return lax.rem(self.sibling + 2 * k, self.peers)


def rows_at(ref, index, rows):
    return ref.at[pl.ds(pl.multiple_of(index * rows, rows), rows)]


class Gather:
    def __init__(self, place, source, out, sems):
        self.place, self.source, self.out = place, source, out
        self.sends, self.forwards, self.arrivals = sems
        self.rows = out.shape[0] // place.peers

    @staticmethod
    def semaphores(peers):
        return [
            pltpu.SemaphoreType.DMA((peers // 2,)),
            pltpu.SemaphoreType.DMA((peers // 2,)),
            pltpu.SemaphoreType.DMA((peers,)),
        ]

    def chunk(self, index):
        return rows_at(self.out, index, self.rows)

    def direct(self, k):
        p = self.place
        return send(self.source, self.chunk(p.me), self.sends.at[k], self.arrivals.at[p.me], "seq", p.mate(k))

    def relayed(self, k):
        p = self.place
        at = p.mate(k)
        src = self.source if k == 0 else self.chunk(at)
        return send(src, self.chunk(at), self.forwards.at[k], self.arrivals.at[at], "seq", p.sibling)

    def arrival(self, index):
        p = self.place
        return send(self.source, self.chunk(index), self.sends.at[0], self.arrivals.at[index], "seq", p.sibling)

    def start(self):
        for k in range(1, self.place.chips):
            self.direct(k).start()
        self.relayed(0).start()

    def relay(self):
        for k in range(1, self.place.chips):
            self.arrival(self.place.mate(k)).wait_recv()
            self.relayed(k).start()

    def finish(self):
        p = self.place
        for k in range(p.chips):
            self.arrival(p.mate_of_sibling(k)).wait_recv()
        for k in range(1, p.chips):
            self.direct(k).wait_send()
        for k in range(p.chips):
            self.relayed(k).wait_send()


class Scatter:
    def __init__(self, place, source, scratch):
        self.place, self.source = place, source
        self.from_sibling, self.summed, self.landed = scratch[:3]
        self.pair_send, self.pair_recv, self.far_send, self.far_recv = scratch[3:]

    @staticmethod
    def scratch(peers, *chunk):
        chips = peers // 2
        return [pltpu.VMEM((chips, *chunk), BF16)] * 3 + [pltpu.SemaphoreType.DMA((chips,))] * 4

    def pair(self, i):
        p = self.place
        return send(
            self.source.at[2 * i + 1 - p.core],
            self.from_sibling.at[i],
            self.pair_send.at[i],
            self.pair_recv.at[i],
            "seq",
            p.sibling,
        )

    def far(self, k):
        p = self.place
        return send(
            self.summed.at[k], self.landed.at[k], self.far_send.at[k], self.far_recv.at[k], "seq", p.mate(k)
        )

    def pair_total(self, i):
        p = self.place
        self.pair(i).wait_recv()
        return self.source[2 * i + p.core].astype(F32) + self.from_sibling[i].astype(F32)

    def start(self):
        for k in range(self.place.chips):
            self.pair(lax.rem(self.place.chip + 1 + k, self.place.chips)).start()

    def combine(self):
        p = self.place
        for k in range(1, p.chips):
            self.summed[k] = self.pair_total(lax.rem(p.chip + k, p.chips)).astype(BF16)
            self.far(k).start()

    def total(self):
        p = self.place
        total = self.pair_total(p.chip)
        for k in range(1, p.chips):
            self.far(k).wait_recv()
            total = total + self.landed[k].astype(F32)
        return total

    def finish(self):
        for i in range(self.place.chips):
            self.pair(i).wait_send()
        for k in range(1, self.place.chips):
            self.far(k).wait_send()


SUB = 2
AHEAD = 3


class LineSum:
    def __init__(self, residual, total, scratch, produce, consume):
        self.residual, self.total = residual, total
        self.landed, self.summed, self.other = scratch[:3]
        self.in_send, self.in_recv, self.swap_recv, self.back_send, self.back_recv = scratch[3:]
        self.produce, self.consume = produce, consume
        self.count, self.rows, self.width = self.summed.shape
        self.n = lax.axis_size("head")
        self.z = lax.axis_index("head")
        low = self.z < self.n // 2
        self.depth = jnp.where(low, self.z, self.n - 1 - self.z)
        self.inward = jnp.where(low, self.z + 1, self.z - 1)
        self.outward = jnp.where(low, self.z - 1, self.z + 1)
        self.inner = self.depth == self.n // 2 - 1
        self.outer = self.depth == 0
        self.lag = self.n // 2 - self.depth + jnp.where(self.outer, AHEAD, 0)
        self.steps = self.count + self.lag

    @staticmethod
    def scratch(count, rows, width):
        sems = pltpu.SemaphoreType.DMA((count, SUB))
        return [pltpu.VMEM((count, rows, width), BF16)] * 3 + [sems] * 5

    def piece(self, j, s):
        size = self.rows // SUB
        return j, pl.ds(s * size, size)

    def up(self, j, s):
        at = self.piece(j, s)
        return send(
            self.summed.at[at], self.landed.at[at], self.in_send.at[j, s], self.in_recv.at[j, s],
            "head", self.inward,
        )

    def swap(self, j, s):
        at = self.piece(j, s)
        return send(
            self.summed.at[at], self.other.at[at], self.in_send.at[j, s], self.swap_recv.at[j, s],
            "head", self.inward,
        )

    def back(self, j, s):
        at = self.piece(j, s)
        return send(
            self.total.at[at], self.total.at[at], self.back_send.at[j, s], self.back_recv.at[j, s],
            "head", self.outward,
        )

    def reduce(self, j):
        part = self.produce(j)
        size = self.rows // SUB
        for s in range(SUB):
            at = self.piece(j, s)
            mine = part[s * size : (s + 1) * size]

            @pl.when(self.outer)
            def _(at=at, mine=mine):
                self.summed[at] = mine.astype(BF16)

            @pl.when(jnp.logical_not(self.outer))
            def _(at=at, mine=mine, s=s):
                self.up(j, s).wait_recv()
                self.summed[at] = (mine + self.landed[at].astype(F32)).astype(BF16)

            @pl.when(self.inner)
            def _(s=s):
                self.swap(j, s).start()

            @pl.when(jnp.logical_not(self.inner))
            def _(s=s):
                self.up(j, s).start()

    def finish_chunk(self, j):
        columns = pl.ds(pl.multiple_of(j * self.width, self.width), self.width)
        size = self.rows // SUB
        for s in range(SUB):
            at = self.piece(j, s)

            @pl.when(self.inner)
            def _(at=at, s=s):
                self.swap(j, s).wait_recv()
                both = self.summed[at].astype(F32) + self.other[at].astype(F32)
                if len(self.residual.shape) == 3:
                    rest = self.residual[at].astype(F32)
                else:
                    rest = self.residual[pl.ds(s * size, size), columns].astype(F32)
                self.total[at] = (rest + both).astype(BF16)

            @pl.when(jnp.logical_not(self.inner))
            def _(s=s):
                self.back(j, s).wait_recv()

            @pl.when(jnp.logical_not(self.outer))
            def _(s=s):
                self.back(j, s).start()

        self.consume(j)

    def run(self, first, last, beside=None):
        def step(t, carry):
            @pl.when(t < self.count)
            def _():
                self.reduce(t)

            @pl.when(t >= self.lag)
            def _():
                self.finish_chunk(t - self.lag)

            if beside is not None:
                beside(t)
            return carry

        lax.fori_loop(first, last, step, 0)

    def finish(self):
        def step(j, carry):
            for s in range(SUB):
                self.up(j, s).wait_send()

                @pl.when(jnp.logical_not(self.outer))
                def _(s=s):
                    self.back(j, s).wait_send()

            return carry

        lax.fori_loop(0, self.count, step, 0)


class Stream:
    def __init__(self, source, held, sem):
        self.source, self.held, self.sem = source, held, sem
        self.count = held.shape[0]

    def copy(self, i):
        return pltpu.make_async_copy(self.source(i), self.held.at[i], self.sem.at[i])

    def start(self):
        for i in range(self.count):
            self.copy(i).start()

    def wait(self, i):
        self.copy(i).wait()


def row_tiles(ref, layer, size):
    if layer is None:
        return lambda i: ref.at[pl.ds(pl.multiple_of(i * size, size), size), :]
    return lambda i: ref.at[layer, pl.ds(pl.multiple_of(i * size, size), size), :]


def column_tiles(ref, layer, size):
    if layer is None:
        return lambda i: ref.at[:, pl.ds(pl.multiple_of(i * size, size), size)]
    return lambda i: ref.at[layer, :, pl.ds(pl.multiple_of(i * size, size), size)]


def meet(seq, head):
    barrier = pltpu.get_barrier_semaphore()
    expected = 0

    def greet(axis, index):
        pl.semaphore_signal(
            barrier, inc=1, device_id={axis: index}, device_id_type=pl.DeviceIdType.MESH
        )

    if seq is not None:
        for k in range(1, seq.chips):
            greet("seq", seq.mate(k))
        greet("seq", seq.sibling)
        expected = seq.chips
    if head:
        n, z = lax.axis_size("head"), lax.axis_index("head")

        @pl.when(z > 0)
        def _():
            greet("head", z - 1)

        @pl.when(z < n - 1)
        def _():
            greet("head", z + 1)

        expected = expected + jnp.where(z > 0, 1, 0) + jnp.where(z < n - 1, 1, 0)
    pl.semaphore_wait(barrier, expected)


def call(kernel, name, number, outs, scratch, *operands, far=0, limit=56):
    whole = pl.BlockSpec(memory_space=pltpu.VMEM)
    return pl.pallas_call(
        kernel,
        out_shape=outs,
        in_specs=[whole] * (len(operands) - far) + [pl.BlockSpec(memory_space=pltpu.HBM)] * far,
        out_specs=jax.tree.map(lambda _: whole, outs),
        scratch_shapes=scratch,
        compiler_params=pltpu.CompilerParams(
            collective_id=number, has_side_effects=True, vmem_limit_bytes=limit * 2**20
        ),
        name=name,
    )(*operands)


def gather_kernel(x_ref, out_ref, *sems):
    place = SeqPlace()
    meet(place, False)
    gather = Gather(place, x_ref, out_ref, sems)
    gather.start()
    out_ref[pl.ds(pl.multiple_of(place.me * gather.rows, gather.rows), gather.rows), :] = x_ref[...]
    gather.relay()
    gather.finish()


def gather_seq(x, name, number):
    peers = lax.axis_size("seq")
    out = jax.ShapeDtypeStruct((peers * x.shape[0], x.shape[1]), x.dtype)
    return call(gather_kernel, name, number, out, Gather.semaphores(peers), x)


def tile_of(width):
    return 256 if width % 256 == 0 else E


def gather_project_kernel(
    second_far, cotangent_far, mid_far, wk_ref, wv_ref, wq_ref, wo_ref,
    out_ref, q1_ref, g1_ref, q0_ref,
    second_ref, cotangent_ref, mid_ref, kv_columns, columns, rows,
    input_sem, kv_sem, column_sem, row_sem, *sems
):
    place = SeqPlace()
    width = q1_ref.shape[1]
    tile = tile_of(width)
    pieces = width // tile
    half = out_ref.shape[1] // 2

    def kv_copy(i):
        return pltpu.make_async_copy((wk_ref, wv_ref)[i], kv_columns.at[i], kv_sem.at[i])

    def column_copy(layer, i):
        return pltpu.make_async_copy(
            wq_ref.at[layer, :, pl.ds(i * tile, tile)], columns.at[layer, i], column_sem.at[layer, i]
        )

    def row_copy(i):
        return pltpu.make_async_copy(wo_ref.at[1, pl.ds(i * tile, tile), :], rows.at[i], row_sem.at[i])

    def input_copy(i):
        source = (mid_far, second_far, cotangent_far)[i]
        return pltpu.make_async_copy(source, (mid_ref, second_ref, cotangent_ref)[i], input_sem.at[i])

    input_copy(0).start()
    for i in range(2):
        kv_copy(i).start()
    input_copy(1).start()
    for i in range(pieces):
        column_copy(1, i).start()
    input_copy(2).start()
    for i in range(pieces):
        row_copy(i).start()
    for i in range(pieces):
        column_copy(0, i).start()
    own = rows_at(out_ref, place.me, out_ref.shape[0] // place.peers)
    gather = Gather(place, own, out_ref, sems)
    input_copy(0).wait()
    for i in range(2):
        kv_copy(i).wait()
        own[:, i * half : (i + 1) * half] = jnp.dot(
            mid_ref[...], kv_columns[i], preferred_element_type=F32
        ).astype(BF16)
    meet(place, False)
    gather.start()
    input_copy(1).wait()
    for i in range(pieces):
        column_copy(1, i).wait()
        q1_ref[:, i * tile : (i + 1) * tile] = jnp.dot(
            second_ref[...], columns[1, i], preferred_element_type=F32
        ).astype(BF16)
    input_copy(2).wait()
    for i in range(pieces):
        row_copy(i).wait()
        g1_ref[:, i * tile : (i + 1) * tile] = contract_last(cotangent_ref[...], rows[i]).astype(BF16)
    for i in range(pieces):
        column_copy(0, i).wait()
        q0_ref[:, i * tile : (i + 1) * tile] = jnp.dot(
            mid_ref[...], columns[0, i], preferred_element_type=F32
        ).astype(BF16)
    gather.relay()
    gather.finish()


def gather_project(second_in, cotangent, mid, w_key, w_value, w_query, w_out):
    peers = lax.axis_size("seq")
    depth, width = w_query.shape[1:]
    tile = tile_of(width)
    pieces = width // tile
    half = w_key.shape[1]
    projected = jax.ShapeDtypeStruct((mid.shape[0], width), BF16)
    outs = (jax.ShapeDtypeStruct((peers * mid.shape[0], 2 * half), BF16),) + (projected,) * 3
    scratch = [
        pltpu.VMEM(second_in.shape, BF16),
        pltpu.VMEM(cotangent.shape, BF16),
        pltpu.VMEM(mid.shape, BF16),
        pltpu.VMEM((2, depth, half), BF16),
        pltpu.VMEM((2, pieces, depth, tile), BF16),
        pltpu.VMEM((pieces, tile, depth), BF16),
        pltpu.SemaphoreType.DMA((3,)),
        pltpu.SemaphoreType.DMA((2,)),
        pltpu.SemaphoreType.DMA((2, pieces)),
        pltpu.SemaphoreType.DMA((pieces,)),
    ] + Gather.semaphores(peers)
    return call(
        gather_project_kernel, "gather_kv", 0, outs, scratch,
        second_in, cotangent, mid, w_key, w_value, w_query, w_out, far=7, limit=52,
    )


class Retention:
    def __init__(self, decay):
        self.decay = decay
        self.count = decay.shape[1]

    def columns(self, h):
        return pl.ds(pl.multiple_of(h * E, E), E)

    def tile(self, ref, h, c):
        return ref[c * RC : (c + 1) * RC, self.columns(h)]

    def row(self, h, c):
        return self.decay[h, c : c + 1, :]

    def across(self, h, c):
        row = jnp.broadcast_to(self.row(h, c), (RC, RC))
        return row, jnp.transpose(row)

    def end(self, h, c):
        return self.row(h, c)[:, RC - 1 : RC]

    def weights(self, row, column):
        later = lax.broadcasted_iota(jnp.int32, (RC, RC), 0)
        lower = later >= lax.broadcasted_iota(jnp.int32, (RC, RC), 1)
        return jnp.where(lower, jnp.exp(jnp.where(lower, column - row, 0.0)), 0.0)


def running_sum(values):
    lane = lax.rem(lax.broadcasted_iota(jnp.int32, values.shape, 1), RC)
    shift = 1
    while shift < RC:
        values = values + jnp.where(lane >= shift, pltpu.roll(values, shift, 1), 0.0)
        shift *= 2
    return values


def first_sum_kernel(
    query_grad, residual, log_decay, ret_query, ret_key, ret_value, wq_ref, wo_ref,
    total, grad_out, accum, second, own_states, states, decays,
    wq, wo, acc, wq_sem, wo_sem, *scratch
):
    place = SeqPlace()
    width = wq.shape[1]
    heads = second.shape[0]
    wq_tiles = Stream(row_tiles(wq_ref, 1, width), wq, wq_sem)
    wo_tiles = Stream(column_tiles(wo_ref, 0, width), wo, wo_sem)
    wq_tiles.start()
    wo_tiles.start()

    def produce(j):
        wq_tiles.wait(j)
        return contract_last(query_grad[...], wq[j])

    def consume(j):
        wo_tiles.wait(j)
        acc[...] += contract_last(total[j], wo[j])

    meet(place, True)
    line = LineSum(residual, total, scratch[:8], produce, consume)
    own_decay = rows_at(decays, place.me, decays.shape[0] // place.peers)
    own_state = rows_at(states, place.me, states.shape[0] // place.peers)
    small = Gather(place, own_decay, decays, scratch[8:11])
    large = Gather(place, own_state, states, scratch[11:14])
    acc[...] = jnp.zeros_like(acc)
    sums = running_sum(log_decay[...])
    for h in range(heads):
        for c in range(accum.shape[1]):
            accum[h, c : c + 1, :] = sums[h : h + 1, c * RC : (c + 1) * RC]
    own_decay[...] = jnp.zeros_like(own_decay)
    ret = Retention(accum)

    def beside(h):
        @pl.when(h < heads)
        def _():
            state = jnp.zeros((E, E), F32)
            decay = jnp.zeros((1, 1), F32)
            for c in range(ret.count):
                row, column = ret.across(h, c)
                end = ret.end(h, c)
                key = ret.tile(ret_key, h, c)
                shrunk = (jnp.exp(end - column) * key.astype(F32)).astype(BF16)
                here = contract_first(shrunk, ret.tile(ret_value, h, c))
                own_states[h, c] = here
                state = jnp.exp(end) * state + here
                decay = decay + end
                products = contract_last(ret.tile(ret_query, h, c), key)
                second[h, c] = (ret.weights(row, column) * products).astype(BF16)
            states[pl.ds(pl.multiple_of((place.me * heads + h) * E, E), E), :] = state.astype(BF16)
            decays[pl.ds(place.me * own_decay.shape[0] + h, 1), :] = jnp.broadcast_to(decay, (1, E))

    line.run(0, heads, beside)
    small.start()
    large.start()
    line.run(heads, line.steps - 1)
    small.relay()
    large.relay()
    line.run(line.steps - 1, line.steps)
    grad_out[...] = acc[...].astype(BF16)
    small.finish()
    large.finish()
    line.finish()


def first_sum(query_grad, residual, log_decay, ret_query, ret_key, ret_value, w_query, w_out):
    peers = lax.axis_size("seq")
    rows, depth = residual.shape
    heads_width = query_grad.shape[1]
    out_width = w_out.shape[1]
    width = tile_of(depth)
    count = depth // width
    heads = ret_query.shape[1] // E
    blocks = rows // RC
    outs = (
        jax.ShapeDtypeStruct((count, rows, width), BF16),
        jax.ShapeDtypeStruct((rows, out_width), BF16),
        jax.ShapeDtypeStruct((heads, blocks, RC), F32),
        jax.ShapeDtypeStruct((heads, blocks, RC, RC), BF16),
        jax.ShapeDtypeStruct((heads, blocks, E, E), F32),
        jax.ShapeDtypeStruct((peers * heads * E, E), BF16),
        jax.ShapeDtypeStruct((peers * log_decay.shape[0], E), F32),
    )
    scratch = [
        pltpu.VMEM((count, width, heads_width), BF16),
        pltpu.VMEM((count, out_width, width), BF16),
        pltpu.VMEM((rows, out_width), F32),
        pltpu.SemaphoreType.DMA((count,)),
        pltpu.SemaphoreType.DMA((count,)),
    ] + LineSum.scratch(count, rows, width) + Gather.semaphores(peers) + Gather.semaphores(peers)
    return call(
        first_sum_kernel, "first_sum", 1, outs, scratch,
        query_grad, residual, log_decay, ret_query, ret_key, ret_value, w_query, w_out, far=2, limit=26,
    )


def second_sum_kernel(
    kv_part, query_grad, residual, mid,
    accum, second, own_states, states, decays, ret_query, ret_key, ret_value,
    wq_ref, wk_ref, wv_ref, wo_ref,
    grad_mid, totals, grad_query, inner_key, inner_value, own_grads, grads,
    grad_o, entering, total, wq, wk, wv, wo, part, kv_grad, weights, acc,
    wq_sem, wk_sem, wv_sem, wo_sem, *scratch
):
    place = SeqPlace()
    count, rows, width = part.shape
    half = kv_grad.shape[1] // 2
    wq_tiles = Stream(row_tiles(wq_ref, 0, width), wq, wq_sem)
    wk_tiles = Stream(row_tiles(wk_ref, None, width), wk, wk_sem)
    wv_tiles = Stream(row_tiles(wv_ref, None, width), wv, wv_sem)
    wo_tiles = Stream(column_tiles(wo_ref, None, width), wo, wo_sem)
    for tiles in (wq_tiles, wk_tiles, wv_tiles, wo_tiles):
        tiles.start()

    def produce(j):
        wk_tiles.wait(j)
        wv_tiles.wait(j)
        return (
            part[j]
            + contract_last(kv_grad[:, :half], wk[j])
            + contract_last(kv_grad[:, half:], wv[j])
        )

    def consume(j):
        wo_tiles.wait(j)
        acc[...] += contract_last(total[j], wo[j])

    def lower(j, carry):
        wq_tiles.wait(j)
        part[j] = contract_last(query_grad[...], wq[j])
        return carry

    meet(place, True)
    scatter_kv = Scatter(place, kv_part, scratch[8:15])
    scatter_kv.start()
    lax.fori_loop(0, 2, lower, 0)
    scatter_kv.combine()
    lax.fori_loop(2, count, lower, 0)
    acc[...] = jnp.zeros_like(acc)
    across = scatter_kv.total()
    for side in (0, 1):
        kv_grad[:, side * half : (side + 1) * half] = jnp.transpose(across[side]).astype(BF16)
    line = LineSum(residual, total, scratch[:8], produce, consume)
    scatter = Scatter(place, weights, scratch[15:22])
    own = rows_at(totals, place.me, totals.shape[0] // place.peers)
    gather = Gather(place, own, totals, scratch[22:25])
    ends = Gather(place, rows_at(grads, place.me, grads.shape[0] // place.peers), grads, scratch[25:28])
    ret = Retention(accum)
    heads = second.shape[0]
    group = decays.shape[0] // place.peers

    def beside(t):
        h = t - late

        @pl.when((h >= 0) & (h < heads))
        def _():
            def hop(s, state):
                grown = jnp.exp(decays[pl.ds(s * group + h, 1), :]) * state
                return grown + states[pl.ds(pl.multiple_of((s * heads + h) * E, E), E), :].astype(F32)

            state = lax.fori_loop(0, place.me, hop, jnp.zeros((E, E), F32))
            for c in range(ret.count):
                entering[h, c] = state.astype(BF16)
                state = jnp.exp(ret.end(h, c)) * state + own_states[h, c]

    def own_grad(h, carry):
        state = jnp.zeros((E, E), F32)
        for c in reversed(range(ret.count)):
            row, column = ret.across(h, c)
            grown = (jnp.exp(column) * ret.tile(ret_query, h, c).astype(F32)).astype(BF16)
            here = contract_first(grown, ret.tile(grad_o, h, c)) * (1.0 / E)
            own_grads[h, c] = here
            state = here + jnp.exp(ret.end(h, c)) * state
        grads[pl.ds(pl.multiple_of((place.me * heads + h) * E, E), E), :] = state.astype(BF16)
        return carry

    def inner(h, carry):
        for c in range(ret.count):
            row, column = ret.across(h, c)
            rows_here = slice(c * RC, (c + 1) * RC)
            grad = ret.tile(grad_o, h, c)
            products = contract_last(grad, ret.tile(ret_value, h, c))
            first = (ret.weights(row, column) * products).astype(BF16)
            near = jnp.dot(first, ret.tile(ret_key, h, c), preferred_element_type=F32)
            carried = contract_last(grad, entering[h, c])
            grad_query[rows_here, ret.columns(h)] = (
                (near + jnp.exp(column) * carried) * (1.0 / E)
            ).astype(BF16)
            inner_key[rows_here, ret.columns(h)] = contract_first(first, ret.tile(ret_query, h, c)) * (1.0 / E)
            inner_value[rows_here, ret.columns(h)] = contract_first(second[h, c], grad) * (1.0 / E)
        return carry

    early = line.lag - 1
    late = line.steps - 1 - heads
    line.run(0, early)
    size = weights.shape[1]
    for i in range(place.peers):
        weights[i] = contract_first(mid[:, i * size : (i + 1) * size], kv_grad[...]).astype(BF16)
    scatter.start()
    line.run(early, early + 2)
    scatter.combine()
    line.run(early + 2, early + 7, beside)
    own[...] = scatter.total().astype(BF16)
    gather.start()
    line.run(early + 7, line.steps - 1, beside)
    gather.relay()
    line.run(line.steps - 1, line.steps)
    grad_o[...] = acc[...].astype(BF16)
    lax.fori_loop(0, heads, own_grad, 0)
    ends.start()
    for j in range(count):
        grad_mid[:, j * width : (j + 1) * width] = total[j]
    lax.fori_loop(0, heads, inner, 0)
    gather.finish()
    scatter.finish()
    ends.relay()
    ends.finish()
    scatter_kv.finish()
    line.finish()


def second_sum(kv_part, query_grad, residual, mid, kept, ret_query, ret_key, ret_value, w_query, w_key, w_value, w_ret_out):
    peers = lax.axis_size("seq")
    rows, depth = mid.shape
    heads_width = query_grad.shape[1]
    out_width = w_ret_out.shape[0]
    both = 2 * w_key.shape[1]
    width = tile_of(depth)
    count = depth // width
    outs = (
        jax.ShapeDtypeStruct((rows, depth), BF16),
        jax.ShapeDtypeStruct((depth, both), BF16),
        jax.ShapeDtypeStruct((rows, out_width), BF16),
        jax.ShapeDtypeStruct((rows, out_width), F32),
        jax.ShapeDtypeStruct((rows, out_width), F32),
        jax.ShapeDtypeStruct(kept[2].shape, F32),
        jax.ShapeDtypeStruct(kept[3].shape, BF16),
    )
    scratch = [
        pltpu.VMEM((rows, out_width), BF16),
        pltpu.VMEM(kept[2].shape, BF16),
        pltpu.VMEM((count, rows, width), BF16),
        pltpu.VMEM((count, width, heads_width), BF16),
        pltpu.VMEM((count, width, both // 2), BF16),
        pltpu.VMEM((count, width, both // 2), BF16),
        pltpu.VMEM((count, out_width, width), BF16),
        pltpu.VMEM((count, rows, width), F32),
        pltpu.VMEM((rows, both), BF16),
        pltpu.VMEM((peers, depth // peers, both), BF16),
        pltpu.VMEM((rows, out_width), F32),
    ] + [pltpu.SemaphoreType.DMA((count,))] * 4
    scratch += (
        LineSum.scratch(count, rows, width)
        + Scatter.scratch(peers, *kv_part.shape[1:])
        + Scatter.scratch(peers, depth // peers, both)
        + Gather.semaphores(peers)
        + Gather.semaphores(peers)
    )
    return call(
        second_sum_kernel, "second_sum", 3, outs, scratch,
        kv_part, query_grad, residual, mid, *kept, ret_query, ret_key, ret_value,
        w_query, w_key, w_value, w_ret_out, far=4, limit=41,
    )


def last_kernel(
    accum, decays, grads, own_grads, inner_key, inner_value, ret_key, ret_value, totals,
    grad_key, grad_value, grad_w_key, grad_w_value, wide, sems
):
    place = SeqPlace()
    ret = Retention(accum)
    heads = own_grads.shape[0]
    group = decays.shape[0] // place.peers
    pieces, size, half = wide.shape[1:]

    def copy(side, i):
        out = (grad_w_key, grad_w_value)[side]
        return pltpu.make_async_copy(wide.at[side, i], out.at[pl.ds(i * size, size)], sems.at[side, i])

    for i in range(pieces):
        for side in (0, 1):
            wide[side, i] = totals[i * size : (i + 1) * size, side * half : (side + 1) * half].astype(F32)
            copy(side, i).start()

    def head(h, carry):
        def hop(k, state):
            s = place.peers - 1 - k
            here = grads[pl.ds(pl.multiple_of((s * heads + h) * E, E), E), :].astype(F32)
            return here + jnp.exp(decays[pl.ds(s * group + h, 1), :]) * state

        state = lax.fori_loop(0, place.peers - 1 - place.me, hop, jnp.zeros((E, E), F32))
        for c in reversed(range(ret.count)):
            rows_here = slice(c * RC, (c + 1) * RC)
            row, column = ret.across(h, c)
            end = ret.end(h, c)
            after = state.astype(BF16)
            shrink = jnp.exp(end - column)
            at_key = contract_last(ret.tile(ret_value, h, c), after)
            at_value = jnp.dot(ret.tile(ret_key, h, c), after, preferred_element_type=F32)
            grad_key[rows_here, ret.columns(h)] = (
                inner_key[rows_here, ret.columns(h)] + shrink * at_key
            ).astype(BF16)
            grad_value[rows_here, ret.columns(h)] = (
                inner_value[rows_here, ret.columns(h)] + shrink * at_value
            ).astype(BF16)
            state = own_grads[h, c] + jnp.exp(end) * state
        return carry

    lax.fori_loop(0, heads, head, 0)
    for i in range(pieces):
        for side in (0, 1):
            copy(side, i).wait()


def last(accum, decays, grads, own_grads, inner_key, inner_value, ret_key, ret_value, totals):
    depth, both = totals.shape
    pieces = 6 if depth % (6 * E) == 0 else 1
    whole = pl.BlockSpec(memory_space=pltpu.VMEM)
    far = pl.BlockSpec(memory_space=pltpu.HBM)
    wide = jax.ShapeDtypeStruct((depth, both // 2), F32)
    narrow = jax.ShapeDtypeStruct(ret_key.shape, BF16)
    return pl.pallas_call(
        last_kernel,
        out_shape=(narrow, narrow, wide, wide),
        in_specs=[whole] * 9,
        out_specs=(whole, whole, far, far),
        scratch_shapes=[
            pltpu.VMEM((2, pieces, depth // pieces, both // 2), F32),
            pltpu.SemaphoreType.DMA((2, pieces)),
        ],
        compiler_params=pltpu.CompilerParams(vmem_limit_bytes=24 * 2**20),
        name="last",
    )(accum, decays, grads, own_grads, inner_key, inner_value, ret_key, ret_value, totals)


def attention_kernel(group, has_prev, mask_ref, *refs):
    if has_prev:
        q_ref, g_ref, k_ref, v_ref, prev_ref, dq_ref, dkv_ref, s_ref, acc = refs
    else:
        q_ref, g_ref, k_ref, v_ref, dq_ref, dkv_ref, s_ref = refs
        acc = dkv_ref
    step = acc.shape[3]
    factor = 1.0 / math.sqrt(E)
    power = factor * math.log2(math.e)
    block = pl.program_id(1)
    first_row = mask_ref[0] + block * BLK
    first_key = mask_ref[1 + block]
    rows = group * BLK

    @pl.when(block == 0)
    def _():
        if has_prev:
            acc[...] = prev_ref[...]
        else:
            acc[...] = jnp.zeros_like(acc)

    q = jnp.concatenate([q_ref[:, i * E : (i + 1) * E] for i in range(group)], axis=0)
    g = jnp.concatenate([g_ref[:, i * E : (i + 1) * E] for i in range(group)], axis=0)
    q_across, g_across = jnp.transpose(q), jnp.transpose(g)
    low = first_key // step
    high = (first_row + BLK + step - 1) // step

    def span(j):
        return pl.ds(pl.multiple_of(j * step, step), step)

    def fold(values, combine):
        total = values[:, :E]
        for i in range(1, step // E):
            total = combine(total, values[:, i * E : (i + 1) * E])
        return total

    def score(masked, j, top):
        scores = contract_last(q, k_ref[span(j), :])
        if masked:
            at = j * step + lax.broadcasted_iota(jnp.int32, (BLK, step), 1)
            query_position = first_row + lax.broadcasted_iota(jnp.int32, (BLK, step), 0)
            seen = (at >= first_key) & (at <= query_position)
            seen = jnp.concatenate([seen] * group, axis=0)
            scores = jnp.where(seen, scores, -jnp.inf)
        s_ref[:, span(j)] = scores
        return jnp.maximum(top, fold(scores, jnp.maximum))

    inside, outside = functools.partial(score, False), functools.partial(score, True)
    top = outside(low, jnp.full((rows, E), -jnp.inf, F32))
    top = lax.fori_loop(low + 1, high - 1, inside, top)
    top = lax.fori_loop(jnp.maximum(low + 1, high - 1), high, outside, top)
    top = jnp.max(top, axis=-1, keepdims=True)

    def raise_(j, total):
        raised = jnp.exp2((s_ref[:, span(j)] - top) * power)
        s_ref[:, span(j)] = raised
        return total + fold(raised, jnp.add)

    total = lax.fori_loop(low, high, raise_, jnp.zeros((rows, E), F32))
    scale = 1.0 / jnp.sum(total, axis=-1, keepdims=True)

    def output(j, out):
        probs = (s_ref[:, span(j)] * scale).astype(BF16)
        return out + jnp.dot(probs, v_ref[span(j), :], preferred_element_type=F32)

    out = lax.fori_loop(low, high, output, jnp.zeros((rows, E), F32)).astype(BF16)
    delta = jnp.sum(g.astype(F32) * out.astype(F32), axis=-1, keepdims=True)

    def back(j, dq):
        probs = s_ref[:, span(j)] * scale
        dprobs = contract_last(g, v_ref[span(j), :])
        dscores = (probs * (dprobs - delta) * factor).astype(BF16)
        acc[j, 0] += jnp.dot(q_across, dscores, preferred_element_type=F32)
        acc[j, 1] += jnp.dot(g_across, probs.astype(BF16), preferred_element_type=F32)
        return dq + jnp.dot(dscores, k_ref[span(j), :], preferred_element_type=F32)

    dq = lax.fori_loop(low, high, back, jnp.zeros((rows, E), F32)).astype(BF16)
    for i in range(group):
        dq_ref[:, i * E : (i + 1) * E] = dq[i * BLK : (i + 1) * BLK, :]
    if has_prev:

        @pl.when(block == pl.num_programs(1) - 1)
        def _():
            dkv_ref[...] = acc[...].astype(BF16)


def attention(mask, queries, grad_out, kv, previous):
    row_count, width = queries.shape
    key_count, both = kv.shape
    heads = both // (2 * E)
    group = width // (heads * E)
    step = row_count
    count = key_count // step
    has_prev = previous is not None
    tile = pl.BlockSpec((BLK, group * E), lambda h, b, m: (b, h))
    key_block = pl.BlockSpec((key_count, E), lambda h, b, m: (0, h))
    value_block = pl.BlockSpec((key_count, E), lambda h, b, m: (0, h + heads))
    part_block = pl.BlockSpec((count, 2, E, step), lambda h, b, m: (0, 0, h, 0))
    part = jax.ShapeDtypeStruct((count, 2, heads * E, step), BF16 if has_prev else F32)
    scratch = [pltpu.VMEM((group * BLK, key_count), F32)]
    if has_prev:
        scratch += [pltpu.VMEM((count, 2, E, step), F32)]
    return pl.pallas_call(
        functools.partial(attention_kernel, group, has_prev),
        out_shape=(jax.ShapeDtypeStruct((row_count, width), BF16), part),
        grid_spec=pltpu.PrefetchScalarGridSpec(
            num_scalar_prefetch=1,
            grid=(heads, row_count // BLK),
            in_specs=[tile, tile, key_block, value_block] + [part_block] * (1 if has_prev else 0),
            out_specs=(tile, part_block),
            scratch_shapes=scratch,
        ),
        compiler_params=pltpu.CompilerParams(vmem_limit_bytes=20 * 2**20),
        cost_estimate=pl.CostEstimate(
            flops=10 * row_count * width * key_count, bytes_accessed=8 * 2**20, transcendentals=0
        ),
        name="attention_back",
    )(mask, queries, grad_out, kv, kv, *(() if previous is None else (previous,)))


def local(
    mid,
    second_in,
    cotangent,
    w_key,
    w_value,
    w_query,
    w_out,
    w_ret_out,
    ret_query,
    ret_key,
    ret_value,
    gate,
    decay_exp,
    mask_start,
):
    row_count = mid.shape[0]
    position = lax.axis_index("seq")
    rate = jnp.exp2(-decay_exp.astype(F32) / 64.0)
    log_decay = jnp.pad(-rate[:, None] * gate, ((0, -gate.shape[0] % 8), (0, 0)))
    kv, queries, grad_out, lower_queries = gather_project(
        second_in, cotangent, mid, w_key, w_value, w_query, w_out
    )
    mask = jnp.concatenate([(position * row_count)[None].astype(jnp.int32), mask_start])

    query_grad, upper = attention(mask, queries, grad_out, kv, None)
    upstream, grad_out, *kept = first_sum(
        query_grad, cotangent, log_decay, ret_query, ret_key, ret_value, w_query, w_out
    )
    query_grad, kv_part = attention(mask, lower_queries, grad_out, kv, upper)
    grad_mid, totals, grad_query, inner_key, inner_value, own_grads, grads = second_sum(
        kv_part, query_grad, upstream, mid,
        kept, ret_query, ret_key, ret_value, w_query, w_key, w_value, w_ret_out,
    )
    grad_key, grad_value, grad_w_key, grad_w_value = last(
        kept[0], kept[4], grads, own_grads, inner_key, inner_value, ret_key, ret_value, totals
    )
    return (grad_mid, grad_query, grad_key, grad_value, grad_w_key, grad_w_value)


def solution(mesh):
    placed = (
        P("seq", None),
        P("seq", None),
        P("seq", None),
        P(None, "head"),
        P(None, "head"),
        P(None, None, "head"),
        P(None, "head", None),
        P("head", None),
        P("seq", "head"),
        P("seq", "head"),
        P("seq", "head"),
        P("head", "seq"),
        P("head"),
        P("seq"),
    )
    return jax.shard_map(
        local,
        mesh=mesh,
        in_specs=placed,
        out_specs=(
            P("seq", None),
            P("seq", "head"),
            P("seq", "head"),
            P("seq", "head"),
            P(None, "head"),
            P(None, "head"),
        ),
        check_vma=False,
    )
```

```python
import functools
import math

import jax
import jax.numpy as jnp
from jax import lax
from jax.experimental import pallas as pl
from jax.experimental.pallas import tpu as pltpu
from jax.sharding import PartitionSpec as P

E = 128
BLK = 128
RC = 128
F32 = jnp.float32
BF16 = jnp.bfloat16


def contract_last(left, right):
    return lax.dot_general(left, right, (((1,), (1,)), ((), ())), preferred_element_type=F32)


def contract_first(left, right):
    return lax.dot_general(left, right, (((0,), (0,)), ((), ())), preferred_element_type=F32)


def send(src, dst, send_sem, recv_sem, axis, index):
    return pltpu.make_async_remote_copy(
        src_ref=src,
        dst_ref=dst,
        send_sem=send_sem,
        recv_sem=recv_sem,
        device_id={axis: index},
        device_id_type=pl.DeviceIdType.MESH,
    )


class SeqPlace:
    def __init__(self):
        self.peers = lax.axis_size("seq")
        self.chips = self.peers // 2
        self.me = lax.axis_index("seq")
        self.chip = self.me // 2
        self.core = lax.rem(self.me, 2)
        self.sibling = self.me + 1 - 2 * self.core

    def mate(self, k):
        return lax.rem(self.me + 2 * k, self.peers)

    def mate_of_sibling(self, k):
        return lax.rem(self.sibling + 2 * k, self.peers)


def rows_at(ref, index, rows):
    return ref.at[pl.ds(pl.multiple_of(index * rows, rows), rows)]


class Gather:
    def __init__(self, place, source, out, sems):
        self.place, self.source, self.out = place, source, out
        self.sends, self.forwards, self.arrivals = sems
        self.rows = out.shape[0] // place.peers

    @staticmethod
    def semaphores(peers):
        return [
            pltpu.SemaphoreType.DMA((peers // 2,)),
            pltpu.SemaphoreType.DMA((peers // 2,)),
            pltpu.SemaphoreType.DMA((peers,)),
        ]

    def chunk(self, index):
        return rows_at(self.out, index, self.rows)

    def direct(self, k):
        p = self.place
        return send(self.source, self.chunk(p.me), self.sends.at[k], self.arrivals.at[p.me], "seq", p.mate(k))

    def relayed(self, k):
        p = self.place
        at = p.mate(k)
        src = self.source if k == 0 else self.chunk(at)
        return send(src, self.chunk(at), self.forwards.at[k], self.arrivals.at[at], "seq", p.sibling)

    def arrival(self, index):
        p = self.place
        return send(self.source, self.chunk(index), self.sends.at[0], self.arrivals.at[index], "seq", p.sibling)

    def start(self):
        for k in range(1, self.place.chips):
            self.direct(k).start()
        self.relayed(0).start()

    def relay(self):
        for k in range(1, self.place.chips):
            self.arrival(self.place.mate(k)).wait_recv()
            self.relayed(k).start()

    def finish(self):
        p = self.place
        for k in range(p.chips):
            self.arrival(p.mate_of_sibling(k)).wait_recv()
        for k in range(1, p.chips):
            self.direct(k).wait_send()
        for k in range(p.chips):
            self.relayed(k).wait_send()


class Scatter:
    def __init__(self, place, source, scratch):
        self.place, self.source = place, source
        self.from_sibling, self.summed, self.landed = scratch[:3]
        self.pair_send, self.pair_recv, self.far_send, self.far_recv = scratch[3:]

    @staticmethod
    def scratch(peers, *chunk):
        chips = peers // 2
        return [pltpu.VMEM((chips, *chunk), BF16)] * 3 + [pltpu.SemaphoreType.DMA((chips,))] * 4

    def pair(self, i):
        p = self.place
        return send(
            self.source.at[2 * i + 1 - p.core],
            self.from_sibling.at[i],
            self.pair_send.at[i],
            self.pair_recv.at[i],
            "seq",
            p.sibling,
        )

    def far(self, k):
        p = self.place
        return send(
            self.summed.at[k], self.landed.at[k], self.far_send.at[k], self.far_recv.at[k], "seq", p.mate(k)
        )

    def pair_total(self, i):
        p = self.place
        self.pair(i).wait_recv()
        return self.source[2 * i + p.core].astype(F32) + self.from_sibling[i].astype(F32)

    def start(self):
        for k in range(self.place.chips):
            self.pair(lax.rem(self.place.chip + 1 + k, self.place.chips)).start()

    def combine(self):
        p = self.place
        for k in range(1, p.chips):
            self.summed[k] = self.pair_total(lax.rem(p.chip + k, p.chips)).astype(BF16)
            self.far(k).start()

    def total(self):
        p = self.place
        total = self.pair_total(p.chip)
        for k in range(1, p.chips):
            self.far(k).wait_recv()
            total = total + self.landed[k].astype(F32)
        return total

    def finish(self):
        for i in range(self.place.chips):
            self.pair(i).wait_send()
        for k in range(1, self.place.chips):
            self.far(k).wait_send()


SUB = 2
AHEAD = 3


class LineSum:
    def __init__(self, residual, total, scratch, produce, consume):
        self.residual, self.total = residual, total
        self.landed, self.summed, self.other = scratch[:3]
        self.in_send, self.in_recv, self.swap_recv, self.back_send, self.back_recv = scratch[3:]
        self.produce, self.consume = produce, consume
        self.count, self.rows, self.width = self.summed.shape
        self.n = lax.axis_size("head")
        self.z = lax.axis_index("head")
        low = self.z < self.n // 2
        self.depth = jnp.where(low, self.z, self.n - 1 - self.z)
        self.inward = jnp.where(low, self.z + 1, self.z - 1)
        self.outward = jnp.where(low, self.z - 1, self.z + 1)
        self.inner = self.depth == self.n // 2 - 1
        self.outer = self.depth == 0
        self.lag = self.n // 2 - self.depth + jnp.where(self.outer, AHEAD, 0)
        self.steps = self.count + self.lag

    @staticmethod
    def scratch(count, rows, width):
        sems = pltpu.SemaphoreType.DMA((count, SUB))
        return [pltpu.VMEM((count, rows, width), BF16)] * 3 + [sems] * 5

    def piece(self, j, s):
        size = self.rows // SUB
        return j, pl.ds(s * size, size)

    def up(self, j, s):
        at = self.piece(j, s)
        return send(
            self.summed.at[at], self.landed.at[at], self.in_send.at[j, s], self.in_recv.at[j, s],
            "head", self.inward,
        )

    def swap(self, j, s):
        at = self.piece(j, s)
        return send(
            self.summed.at[at], self.other.at[at], self.in_send.at[j, s], self.swap_recv.at[j, s],
            "head", self.inward,
        )

    def back(self, j, s):
        at = self.piece(j, s)
        return send(
            self.total.at[at], self.total.at[at], self.back_send.at[j, s], self.back_recv.at[j, s],
            "head", self.outward,
        )

    def reduce(self, j):
        part = self.produce(j)
        size = self.rows // SUB
        for s in range(SUB):
            at = self.piece(j, s)
            mine = part[s * size : (s + 1) * size]

            @pl.when(self.outer)
            def _(at=at, mine=mine):
                self.summed[at] = mine.astype(BF16)

            @pl.when(jnp.logical_not(self.outer))
            def _(at=at, mine=mine, s=s):
                self.up(j, s).wait_recv()
                self.summed[at] = (mine + self.landed[at].astype(F32)).astype(BF16)

            @pl.when(self.inner)
            def _(s=s):
                self.swap(j, s).start()

            @pl.when(jnp.logical_not(self.inner))
            def _(s=s):
                self.up(j, s).start()

    def finish_chunk(self, j):
        columns = pl.ds(pl.multiple_of(j * self.width, self.width), self.width)
        size = self.rows // SUB
        for s in range(SUB):
            at = self.piece(j, s)

            @pl.when(self.inner)
            def _(at=at, s=s):
                self.swap(j, s).wait_recv()
                both = self.summed[at].astype(F32) + self.other[at].astype(F32)
                if len(self.residual.shape) == 3:
                    rest = self.residual[at].astype(F32)
                else:
                    rest = self.residual[pl.ds(s * size, size), columns].astype(F32)
                self.total[at] = (rest + both).astype(BF16)

            @pl.when(jnp.logical_not(self.inner))
            def _(s=s):
                self.back(j, s).wait_recv()

            @pl.when(jnp.logical_not(self.outer))
            def _(s=s):
                self.back(j, s).start()

        self.consume(j)

    def run(self, first, last, beside=None):
        def step(t, carry):
            @pl.when(t < self.count)
            def _():
                self.reduce(t)

            @pl.when(t >= self.lag)
            def _():
                self.finish_chunk(t - self.lag)

            if beside is not None:
                beside(t)
            return carry

        lax.fori_loop(first, last, step, 0)

    def finish(self):
        def step(j, carry):
            for s in range(SUB):
                self.up(j, s).wait_send()

                @pl.when(jnp.logical_not(self.outer))
                def _(s=s):
                    self.back(j, s).wait_send()

            return carry

        lax.fori_loop(0, self.count, step, 0)


class Stream:
    def __init__(self, source, held, sem):
        self.source, self.held, self.sem = source, held, sem
        self.count = held.shape[0]

    def copy(self, i):
        return pltpu.make_async_copy(self.source(i), self.held.at[i], self.sem.at[i])

    def start(self):
        for i in range(self.count):
            self.copy(i).start()

    def wait(self, i):
        self.copy(i).wait()


def row_tiles(ref, layer, size):
    if layer is None:
        return lambda i: ref.at[pl.ds(pl.multiple_of(i * size, size), size), :]
    return lambda i: ref.at[layer, pl.ds(pl.multiple_of(i * size, size), size), :]


def column_tiles(ref, layer, size):
    if layer is None:
        return lambda i: ref.at[:, pl.ds(pl.multiple_of(i * size, size), size)]
    return lambda i: ref.at[layer, :, pl.ds(pl.multiple_of(i * size, size), size)]


def meet(seq, head):
    barrier = pltpu.get_barrier_semaphore()
    expected = 0

    def greet(axis, index):
        pl.semaphore_signal(
            barrier, inc=1, device_id={axis: index}, device_id_type=pl.DeviceIdType.MESH
        )

    if seq is not None:
        for k in range(1, seq.chips):
            greet("seq", seq.mate(k))
        greet("seq", seq.sibling)
        expected = seq.chips
    if head:
        n, z = lax.axis_size("head"), lax.axis_index("head")

        @pl.when(z > 0)
        def _():
            greet("head", z - 1)

        @pl.when(z < n - 1)
        def _():
            greet("head", z + 1)

        expected = expected + jnp.where(z > 0, 1, 0) + jnp.where(z < n - 1, 1, 0)
    pl.semaphore_wait(barrier, expected)


def call(kernel, name, number, outs, scratch, *operands, far=0, limit=56, near=0):
    whole = pl.BlockSpec(memory_space=pltpu.VMEM)
    return pl.pallas_call(
        kernel,
        out_shape=outs,
        in_specs=[pl.BlockSpec(memory_space=pltpu.SMEM)] * near
        + [whole] * (len(operands) - far - near)
        + [pl.BlockSpec(memory_space=pltpu.HBM)] * far,
        out_specs=jax.tree.map(lambda _: whole, outs),
        scratch_shapes=scratch,
        compiler_params=pltpu.CompilerParams(
            collective_id=number, has_side_effects=True, vmem_limit_bytes=limit * 2**20
        ),
        name=name,
    )(*operands)


def gather_kernel(x_ref, out_ref, *sems):
    place = SeqPlace()
    meet(place, False)
    gather = Gather(place, x_ref, out_ref, sems)
    gather.start()
    out_ref[pl.ds(pl.multiple_of(place.me * gather.rows, gather.rows), gather.rows), :] = x_ref[...]
    gather.relay()
    gather.finish()


def gather_seq(x, name, number):
    peers = lax.axis_size("seq")
    out = jax.ShapeDtypeStruct((peers * x.shape[0], x.shape[1]), x.dtype)
    return call(gather_kernel, name, number, out, Gather.semaphores(peers), x)


def tile_of(width):
    return 256 if width % 256 == 0 else E


def gather_project_kernel(
    second_far, cotangent_far, mid_far, wk_ref, wv_ref, wq_ref, wo_ref,
    out_ref, q1_ref, g1_ref, q0_ref,
    second_ref, cotangent_ref, mid_ref, kv_columns, columns, rows,
    input_sem, kv_sem, column_sem, row_sem, *sems
):
    place = SeqPlace()
    width = q1_ref.shape[1]
    tile = tile_of(width)
    pieces = width // tile
    half = out_ref.shape[1] // 2

    def kv_copy(i):
        return pltpu.make_async_copy((wk_ref, wv_ref)[i], kv_columns.at[i], kv_sem.at[i])

    def column_copy(layer, i):
        return pltpu.make_async_copy(
            wq_ref.at[layer, :, pl.ds(i * tile, tile)], columns.at[layer, i], column_sem.at[layer, i]
        )

    def row_copy(i):
        return pltpu.make_async_copy(wo_ref.at[1, pl.ds(i * tile, tile), :], rows.at[i], row_sem.at[i])

    def input_copy(i):
        source = (mid_far, second_far, cotangent_far)[i]
        return pltpu.make_async_copy(source, (mid_ref, second_ref, cotangent_ref)[i], input_sem.at[i])

    input_copy(0).start()
    for i in range(2):
        kv_copy(i).start()
    input_copy(1).start()
    for i in range(pieces):
        column_copy(1, i).start()
    input_copy(2).start()
    for i in range(pieces):
        row_copy(i).start()
    for i in range(pieces):
        column_copy(0, i).start()
    own = rows_at(out_ref, place.me, out_ref.shape[0] // place.peers)
    gather = Gather(place, own, out_ref, sems)
    input_copy(0).wait()
    for i in range(2):
        kv_copy(i).wait()
        own[:, i * half : (i + 1) * half] = jnp.dot(
            mid_ref[...], kv_columns[i], preferred_element_type=F32
        ).astype(BF16)
    meet(place, False)
    gather.start()
    input_copy(1).wait()
    for i in range(pieces):
        column_copy(1, i).wait()
        q1_ref[:, i * tile : (i + 1) * tile] = jnp.dot(
            second_ref[...], columns[1, i], preferred_element_type=F32
        ).astype(BF16)
    input_copy(2).wait()
    for i in range(pieces):
        row_copy(i).wait()
        g1_ref[:, i * tile : (i + 1) * tile] = contract_last(cotangent_ref[...], rows[i]).astype(BF16)
    for i in range(pieces):
        column_copy(0, i).wait()
        q0_ref[:, i * tile : (i + 1) * tile] = jnp.dot(
            mid_ref[...], columns[0, i], preferred_element_type=F32
        ).astype(BF16)
    gather.relay()
    gather.finish()


def gather_project(second_in, cotangent, mid, w_key, w_value, w_query, w_out):
    peers = lax.axis_size("seq")
    depth, width = w_query.shape[1:]
    tile = tile_of(width)
    pieces = width // tile
    half = w_key.shape[1]
    projected = jax.ShapeDtypeStruct((mid.shape[0], width), BF16)
    outs = (jax.ShapeDtypeStruct((peers * mid.shape[0], 2 * half), BF16),) + (projected,) * 3
    scratch = [
        pltpu.VMEM(second_in.shape, BF16),
        pltpu.VMEM(cotangent.shape, BF16),
        pltpu.VMEM(mid.shape, BF16),
        pltpu.VMEM((2, depth, half), BF16),
        pltpu.VMEM((2, pieces, depth, tile), BF16),
        pltpu.VMEM((pieces, tile, depth), BF16),
        pltpu.SemaphoreType.DMA((3,)),
        pltpu.SemaphoreType.DMA((2,)),
        pltpu.SemaphoreType.DMA((2, pieces)),
        pltpu.SemaphoreType.DMA((pieces,)),
    ] + Gather.semaphores(peers)
    return call(
        gather_project_kernel, "gather_kv", 0, outs, scratch,
        second_in, cotangent, mid, w_key, w_value, w_query, w_out, far=7, limit=52,
    )


class Retention:
    def __init__(self, decay):
        self.decay = decay
        self.count = decay.shape[1]

    def columns(self, h):
        return pl.ds(pl.multiple_of(h * E, E), E)

    def tile(self, ref, h, c):
        return ref[c * RC : (c + 1) * RC, self.columns(h)]

    def row(self, h, c):
        return self.decay[h, c : c + 1, :]

    def across(self, h, c):
        row = jnp.broadcast_to(self.row(h, c), (RC, RC))
        return row, jnp.transpose(row)

    def end(self, h, c):
        return self.row(h, c)[:, RC - 1 : RC]

    def weights(self, row, column):
        later = lax.broadcasted_iota(jnp.int32, (RC, RC), 0)
        lower = later >= lax.broadcasted_iota(jnp.int32, (RC, RC), 1)
        return jnp.where(lower, jnp.exp(jnp.where(lower, column - row, 0.0)), 0.0)


def running_sum(values):
    lane = lax.rem(lax.broadcasted_iota(jnp.int32, values.shape, 1), RC)
    shift = 1
    while shift < RC:
        values = values + jnp.where(lane >= shift, pltpu.roll(values, shift, 1), 0.0)
        shift *= 2
    return values


def first_sum_kernel(
    exponent, query_grad, residual, gate, ret_query, ret_key, ret_value, wq_ref, wo_ref,
    total, grad_out, accum, second, own_states, states, decays,
    logs, wq, wo, acc, wq_sem, wo_sem, *scratch
):
    place = SeqPlace()
    width = wq.shape[1]
    heads = second.shape[0]
    wq_tiles = Stream(row_tiles(wq_ref, 1, width), wq, wq_sem)
    wo_tiles = Stream(column_tiles(wo_ref, 0, width), wo, wo_sem)
    wq_tiles.start()
    wo_tiles.start()

    def produce(j):
        wq_tiles.wait(j)
        return contract_last(query_grad[...], wq[j])

    def consume(j):
        wo_tiles.wait(j)
        acc[...] += contract_last(total[j], wo[j])

    meet(place, True)
    line = LineSum(residual, total, scratch[:8], produce, consume)
    own_decay = rows_at(decays, place.me, decays.shape[0] // place.peers)
    own_state = rows_at(states, place.me, states.shape[0] // place.peers)
    small = Gather(place, own_decay, decays, scratch[8:11])
    large = Gather(place, own_state, states, scratch[11:14])
    acc[...] = jnp.zeros_like(acc)
    for h in range(heads):
        power = jnp.broadcast_to(-exponent[h].astype(F32) / 64.0, (1, gate.shape[1]))
        logs[h : h + 1, :] = -jnp.exp2(power) * gate[h : h + 1, :]
    sums = running_sum(logs[...])
    for h in range(heads):
        for c in range(accum.shape[1]):
            accum[h, c : c + 1, :] = sums[h : h + 1, c * RC : (c + 1) * RC]
    own_decay[...] = jnp.zeros_like(own_decay)
    ret = Retention(accum)

    def beside(h):
        @pl.when(h < heads)
        def _():
            state = jnp.zeros((E, E), F32)
            decay = jnp.zeros((1, 1), F32)
            for c in range(ret.count):
                row, column = ret.across(h, c)
                end = ret.end(h, c)
                key = ret.tile(ret_key, h, c)
                shrunk = (jnp.exp(end - column) * key.astype(F32)).astype(BF16)
                here = contract_first(shrunk, ret.tile(ret_value, h, c))
                own_states[h, c] = here
                state = jnp.exp(end) * state + here
                decay = decay + end
                products = contract_last(ret.tile(ret_query, h, c), key)
                second[h, c] = (ret.weights(row, column) * products).astype(BF16)
            states[pl.ds(pl.multiple_of((place.me * heads + h) * E, E), E), :] = state.astype(BF16)
            decays[pl.ds(place.me * own_decay.shape[0] + h, 1), :] = jnp.broadcast_to(decay, (1, E))

    line.run(0, heads, beside)
    small.start()
    large.start()
    line.run(heads, line.steps - 1)
    small.relay()
    large.relay()
    line.run(line.steps - 1, line.steps)
    grad_out[...] = acc[...].astype(BF16)
    small.finish()
    large.finish()
    line.finish()


def first_sum(decay_exp, query_grad, residual, gate, ret_query, ret_key, ret_value, w_query, w_out):
    peers = lax.axis_size("seq")
    rows, depth = residual.shape
    heads_width = query_grad.shape[1]
    out_width = w_out.shape[1]
    width = tile_of(depth)
    count = depth // width
    heads = ret_query.shape[1] // E
    blocks = rows // RC
    group = heads + -heads % 8
    outs = (
        jax.ShapeDtypeStruct((count, rows, width), BF16),
        jax.ShapeDtypeStruct((rows, out_width), BF16),
        jax.ShapeDtypeStruct((heads, blocks, RC), F32),
        jax.ShapeDtypeStruct((heads, blocks, RC, RC), BF16),
        jax.ShapeDtypeStruct((heads, blocks, E, E), F32),
        jax.ShapeDtypeStruct((peers * heads * E, E), BF16),
        jax.ShapeDtypeStruct((peers * group, E), F32),
    )
    scratch = [
        pltpu.VMEM((group, rows), F32),
        pltpu.VMEM((count, width, heads_width), BF16),
        pltpu.VMEM((count, out_width, width), BF16),
        pltpu.VMEM((rows, out_width), F32),
        pltpu.SemaphoreType.DMA((count,)),
        pltpu.SemaphoreType.DMA((count,)),
    ] + LineSum.scratch(count, rows, width) + Gather.semaphores(peers) + Gather.semaphores(peers)
    return call(
        first_sum_kernel, "first_sum", 1, outs, scratch,
        decay_exp, query_grad, residual, gate, ret_query, ret_key, ret_value, w_query, w_out,
        far=2, limit=22, near=1,
    )


def second_sum_kernel(
    kv_part, query_grad, residual, mid,
    accum, second, own_states, states, decays, ret_query, ret_key, ret_value,
    wq_ref, wk_ref, wv_ref, wo_ref,
    grad_mid, totals, grad_query, inner_key, inner_value, own_grads, grads,
    grad_o, entering, total, wq, wk, wv, wo, part, kv_grad, weights, acc,
    wq_sem, wk_sem, wv_sem, wo_sem, *scratch
):
    place = SeqPlace()
    count, rows, width = part.shape
    half = kv_grad.shape[1] // 2
    wq_tiles = Stream(row_tiles(wq_ref, 0, width), wq, wq_sem)
    wk_tiles = Stream(row_tiles(wk_ref, None, width), wk, wk_sem)
    wv_tiles = Stream(row_tiles(wv_ref, None, width), wv, wv_sem)
    wo_tiles = Stream(column_tiles(wo_ref, None, width), wo, wo_sem)
    for tiles in (wq_tiles, wk_tiles, wv_tiles, wo_tiles):
        tiles.start()

    def produce(j):
        wk_tiles.wait(j)
        wv_tiles.wait(j)
        return (
            part[j]
            + contract_last(kv_grad[:, :half], wk[j])
            + contract_last(kv_grad[:, half:], wv[j])
        )

    def consume(j):
        wo_tiles.wait(j)
        acc[...] += contract_last(total[j], wo[j])

    def lower(j, carry):
        wq_tiles.wait(j)
        part[j] = contract_last(query_grad[...], wq[j])
        return carry

    meet(place, True)
    scatter_kv = Scatter(place, kv_part, scratch[8:15])
    scatter_kv.start()
    lax.fori_loop(0, 2, lower, 0)
    scatter_kv.combine()
    lax.fori_loop(2, count, lower, 0)
    acc[...] = jnp.zeros_like(acc)
    across = scatter_kv.total()
    for side in (0, 1):
        kv_grad[:, side * half : (side + 1) * half] = jnp.transpose(across[side]).astype(BF16)
    line = LineSum(residual, total, scratch[:8], produce, consume)
    scatter = Scatter(place, weights, scratch[15:22])
    own = rows_at(totals, place.me, totals.shape[0] // place.peers)
    gather = Gather(place, own, totals, scratch[22:25])
    ends = Gather(place, rows_at(grads, place.me, grads.shape[0] // place.peers), grads, scratch[25:28])
    ret = Retention(accum)
    heads = second.shape[0]
    group = decays.shape[0] // place.peers

    def beside(t):
        h = t - late

        @pl.when((h >= 0) & (h < heads))
        def _():
            def hop(s, state):
                grown = jnp.exp(decays[pl.ds(s * group + h, 1), :]) * state
                return grown + states[pl.ds(pl.multiple_of((s * heads + h) * E, E), E), :].astype(F32)

            state = lax.fori_loop(0, place.me, hop, jnp.zeros((E, E), F32))
            for c in range(ret.count):
                entering[h, c] = state.astype(BF16)
                state = jnp.exp(ret.end(h, c)) * state + own_states[h, c]

    def own_grad(h, carry):
        state = jnp.zeros((E, E), F32)
        for c in reversed(range(ret.count)):
            row, column = ret.across(h, c)
            grown = (jnp.exp(column) * ret.tile(ret_query, h, c).astype(F32)).astype(BF16)
            here = contract_first(grown, ret.tile(grad_o, h, c)) * (1.0 / E)
            own_grads[h, c] = here
            state = here + jnp.exp(ret.end(h, c)) * state
        grads[pl.ds(pl.multiple_of((place.me * heads + h) * E, E), E), :] = state.astype(BF16)
        return carry

    def inner(h, carry):
        for c in range(ret.count):
            row, column = ret.across(h, c)
            rows_here = slice(c * RC, (c + 1) * RC)
            grad = ret.tile(grad_o, h, c)
            products = contract_last(grad, ret.tile(ret_value, h, c))
            first = (ret.weights(row, column) * products).astype(BF16)
            near = jnp.dot(first, ret.tile(ret_key, h, c), preferred_element_type=F32)
            carried = contract_last(grad, entering[h, c])
            grad_query[rows_here, ret.columns(h)] = (
                (near + jnp.exp(column) * carried) * (1.0 / E)
            ).astype(BF16)
            inner_key[rows_here, ret.columns(h)] = contract_first(first, ret.tile(ret_query, h, c)) * (1.0 / E)
            inner_value[rows_here, ret.columns(h)] = contract_first(second[h, c], grad) * (1.0 / E)
        return carry

    early = line.lag - 1
    late = line.steps - 1 - heads
    line.run(0, early)
    size = weights.shape[1]
    for i in range(place.peers):
        weights[i] = contract_first(mid[:, i * size : (i + 1) * size], kv_grad[...]).astype(BF16)
    scatter.start()
    line.run(early, early + 2)
    scatter.combine()
    line.run(early + 2, early + 9, beside)
    own[...] = scatter.total().astype(BF16)
    gather.start()
    line.run(early + 9, line.steps, beside)
    grad_o[...] = acc[...].astype(BF16)
    lax.fori_loop(0, heads, own_grad, 0)
    ends.start()
    for j in range(count):
        grad_mid[:, j * width : (j + 1) * width] = total[j]
    gather.relay()
    lax.fori_loop(0, heads, inner, 0)
    gather.finish()
    scatter.finish()
    ends.relay()
    ends.finish()
    scatter_kv.finish()
    line.finish()


def second_sum(kv_part, query_grad, residual, mid, kept, ret_query, ret_key, ret_value, w_query, w_key, w_value, w_ret_out):
    peers = lax.axis_size("seq")
    rows, depth = mid.shape
    heads_width = query_grad.shape[1]
    out_width = w_ret_out.shape[0]
    both = 2 * w_key.shape[1]
    width = tile_of(depth)
    count = depth // width
    outs = (
        jax.ShapeDtypeStruct((rows, depth), BF16),
        jax.ShapeDtypeStruct((depth, both), BF16),
        jax.ShapeDtypeStruct((rows, out_width), BF16),
        jax.ShapeDtypeStruct((rows, out_width), F32),
        jax.ShapeDtypeStruct((rows, out_width), F32),
        jax.ShapeDtypeStruct(kept[2].shape, F32),
        jax.ShapeDtypeStruct(kept[3].shape, BF16),
    )
    scratch = [
        pltpu.VMEM((rows, out_width), BF16),
        pltpu.VMEM(kept[2].shape, BF16),
        pltpu.VMEM((count, rows, width), BF16),
        pltpu.VMEM((count, width, heads_width), BF16),
        pltpu.VMEM((count, width, both // 2), BF16),
        pltpu.VMEM((count, width, both // 2), BF16),
        pltpu.VMEM((count, out_width, width), BF16),
        pltpu.VMEM((count, rows, width), F32),
        pltpu.VMEM((rows, both), BF16),
        pltpu.VMEM((peers, depth // peers, both), BF16),
        pltpu.VMEM((rows, out_width), F32),
    ] + [pltpu.SemaphoreType.DMA((count,))] * 4
    scratch += (
        LineSum.scratch(count, rows, width)
        + Scatter.scratch(peers, *kv_part.shape[1:])
        + Scatter.scratch(peers, depth // peers, both)
        + Gather.semaphores(peers)
        + Gather.semaphores(peers)
    )
    return call(
        second_sum_kernel, "second_sum", 3, outs, scratch,
        kv_part, query_grad, residual, mid, *kept, ret_query, ret_key, ret_value,
        w_query, w_key, w_value, w_ret_out, far=4, limit=41,
    )


def last_kernel(
    accum, decays, grads, own_grads, inner_key, inner_value, ret_key, ret_value, totals,
    grad_key, grad_value, grad_w_key, grad_w_value, wide, sems
):
    place = SeqPlace()
    ret = Retention(accum)
    heads = own_grads.shape[0]
    group = decays.shape[0] // place.peers
    pieces, size, half = wide.shape[1:]

    def copy(side, i):
        out = (grad_w_key, grad_w_value)[side]
        return pltpu.make_async_copy(wide.at[side, i], out.at[pl.ds(i * size, size)], sems.at[side, i])

    for i in range(pieces):
        for side in (0, 1):
            wide[side, i] = totals[i * size : (i + 1) * size, side * half : (side + 1) * half].astype(F32)
            copy(side, i).start()

    def head(h, carry):
        def hop(k, state):
            s = place.peers - 1 - k
            here = grads[pl.ds(pl.multiple_of((s * heads + h) * E, E), E), :].astype(F32)
            return here + jnp.exp(decays[pl.ds(s * group + h, 1), :]) * state

        state = lax.fori_loop(0, place.peers - 1 - place.me, hop, jnp.zeros((E, E), F32))
        for c in reversed(range(ret.count)):
            rows_here = slice(c * RC, (c + 1) * RC)
            row, column = ret.across(h, c)
            end = ret.end(h, c)
            after = state.astype(BF16)
            shrink = jnp.exp(end - column)
            at_key = contract_last(ret.tile(ret_value, h, c), after)
            at_value = jnp.dot(ret.tile(ret_key, h, c), after, preferred_element_type=F32)
            grad_key[rows_here, ret.columns(h)] = (
                inner_key[rows_here, ret.columns(h)] + shrink * at_key
            ).astype(BF16)
            grad_value[rows_here, ret.columns(h)] = (
                inner_value[rows_here, ret.columns(h)] + shrink * at_value
            ).astype(BF16)
            state = own_grads[h, c] + jnp.exp(end) * state
        return carry

    lax.fori_loop(0, heads, head, 0)
    for i in range(pieces):
        for side in (0, 1):
            copy(side, i).wait()


def last(accum, decays, grads, own_grads, inner_key, inner_value, ret_key, ret_value, totals):
    depth, both = totals.shape
    pieces = 6 if depth % (6 * E) == 0 else 1
    whole = pl.BlockSpec(memory_space=pltpu.VMEM)
    far = pl.BlockSpec(memory_space=pltpu.HBM)
    wide = jax.ShapeDtypeStruct((depth, both // 2), F32)
    narrow = jax.ShapeDtypeStruct(ret_key.shape, BF16)
    return pl.pallas_call(
        last_kernel,
        out_shape=(narrow, narrow, wide, wide),
        in_specs=[whole] * 9,
        out_specs=(whole, whole, far, far),
        scratch_shapes=[
            pltpu.VMEM((2, pieces, depth // pieces, both // 2), F32),
            pltpu.SemaphoreType.DMA((2, pieces)),
        ],
        compiler_params=pltpu.CompilerParams(vmem_limit_bytes=24 * 2**20),
        name="last",
    )(accum, decays, grads, own_grads, inner_key, inner_value, ret_key, ret_value, totals)


UNROLL = (4, 2, 1)


def sweep(first, last, body, carry):
    for width in UNROLL:
        many = jnp.maximum(last - first, 0) // width

        def several(i, carry, first=first, width=width):
            for k in range(width):
                carry = body(first + width * i + k, carry)
            return carry

        carry = lax.fori_loop(0, many, several, carry)
        first = first + width * many
    return carry


def attention_kernel(group, has_prev, mask_ref, *refs):
    if has_prev:
        q_all, g_all, kv_ref, prev_ref, dq_all, dkv_ref, s_ref, acc_all = refs
        acc_all[...] = prev_ref[...]
    else:
        q_all, g_all, kv_ref, dq_all, dkv_ref, s_ref = refs
        acc_all = dkv_ref
        acc_all[...] = jnp.zeros_like(acc_all)
    heads = acc_all.shape[2] // E
    blocks = q_all.shape[0] // BLK

    def tile(i, carry):
        h, b = i // blocks, lax.rem(i, blocks)
        at = pl.ds(pl.multiple_of(b * BLK, BLK), BLK)
        across = pl.ds(pl.multiple_of(h * group * E, E), group * E)
        here = pl.ds(pl.multiple_of(h * E, E), E)
        attention_tile(
            group, mask_ref, b, q_all.at[at, across], g_all.at[at, across], kv_ref.at[:, here],
            kv_ref.at[:, pl.ds(pl.multiple_of((heads + h) * E, E), E)],
            dq_all.at[at, across], acc_all.at[:, :, here], s_ref,
        )
        return carry

    lax.fori_loop(0, heads * blocks, tile, 0)
    if has_prev:
        dkv_ref[...] = acc_all[...].astype(BF16)


def attention_tile(group, mask_ref, block, q_ref, g_ref, k_ref, v_ref, dq_ref, acc, s_ref):
    step = acc.shape[3]
    factor = 1.0 / math.sqrt(E)
    power = factor * math.log2(math.e)
    first_row = lax.axis_index("seq") * step + block * BLK
    first_key = mask_ref[block]
    rows = group * BLK
    q = jnp.concatenate([q_ref[:, i * E : (i + 1) * E] for i in range(group)], axis=0)
    g = jnp.concatenate([g_ref[:, i * E : (i + 1) * E] for i in range(group)], axis=0)
    q_across, g_across = jnp.transpose(q), jnp.transpose(g)
    low = first_key // step
    high = (first_row + BLK + step - 1) // step

    def span(j):
        return pl.ds(pl.multiple_of(j * step, step), step)

    def fold(values, combine):
        total = values[:, :E]
        for i in range(1, step // E):
            total = combine(total, values[:, i * E : (i + 1) * E])
        return total

    def score(masked, j, top):
        scores = contract_last(q, k_ref[span(j), :])
        if masked:
            at = j * step + lax.broadcasted_iota(jnp.int32, (BLK, step), 1)
            query_position = first_row + lax.broadcasted_iota(jnp.int32, (BLK, step), 0)
            seen = (at >= first_key) & (at <= query_position)
            seen = jnp.concatenate([seen] * group, axis=0)
            scores = jnp.where(seen, scores, -jnp.inf)
        s_ref[:, span(j)] = scores
        return jnp.maximum(top, fold(scores, jnp.maximum))

    inside, outside = functools.partial(score, False), functools.partial(score, True)
    top = outside(low, jnp.full((rows, E), -jnp.inf, F32))
    top = sweep(low + 1, high - 1, inside, top)
    top = lax.fori_loop(jnp.maximum(low + 1, high - 1), high, outside, top)
    top = jnp.max(top, axis=-1, keepdims=True)

    def raise_(j, total):
        raised = jnp.exp2((s_ref[:, span(j)] - top) * power)
        s_ref[:, span(j)] = raised
        return total + fold(raised, jnp.add)

    total = sweep(low, high, raise_, jnp.zeros((rows, E), F32))
    scale = 1.0 / jnp.sum(total, axis=-1, keepdims=True)

    def output(j, out):
        probs = (s_ref[:, span(j)] * scale).astype(BF16)
        return out + jnp.dot(probs, v_ref[span(j), :], preferred_element_type=F32)

    out = sweep(low, high, output, jnp.zeros((rows, E), F32)).astype(BF16)
    delta = jnp.sum(g.astype(F32) * out.astype(F32), axis=-1, keepdims=True)

    def back(j, dq):
        probs = s_ref[:, span(j)] * scale
        dprobs = contract_last(g, v_ref[span(j), :])
        dscores = (probs * (dprobs - delta) * factor).astype(BF16)
        acc[j, 0] += jnp.dot(q_across, dscores, preferred_element_type=F32)
        acc[j, 1] += jnp.dot(g_across, probs.astype(BF16), preferred_element_type=F32)
        return dq + jnp.dot(dscores, k_ref[span(j), :], preferred_element_type=F32)

    dq = sweep(low, high, back, jnp.zeros((rows, E), F32)).astype(BF16)
    for i in range(group):
        dq_ref[:, i * E : (i + 1) * E] = dq[i * BLK : (i + 1) * BLK, :]


def attention(mask_start, queries, grad_out, kv, previous):
    row_count, width = queries.shape
    key_count, both = kv.shape
    heads = both // (2 * E)
    group = width // (heads * E)
    step = row_count
    count = key_count // step
    has_prev = previous is not None
    part = jax.ShapeDtypeStruct((count, 2, heads * E, step), BF16 if has_prev else F32)
    scratch = [pltpu.VMEM((group * BLK, key_count), F32)]
    if has_prev:
        scratch += [pltpu.VMEM(part.shape, F32)]
    whole = pl.BlockSpec(memory_space=pltpu.VMEM)
    return pl.pallas_call(
        functools.partial(attention_kernel, group, has_prev),
        out_shape=(jax.ShapeDtypeStruct((row_count, width), BF16), part),
        in_specs=[pl.BlockSpec(memory_space=pltpu.SMEM)] + [whole] * (4 if has_prev else 3),
        out_specs=(whole, whole),
        scratch_shapes=scratch,
        compiler_params=pltpu.CompilerParams(vmem_limit_bytes=20 * 2**20),
        cost_estimate=pl.CostEstimate(
            flops=10 * row_count * width * key_count, bytes_accessed=8 * 2**20, transcendentals=0
        ),
        name="attention_back",
    )(mask_start, queries, grad_out, kv, *(() if previous is None else (previous,)))


def local(
    mid,
    second_in,
    cotangent,
    w_key,
    w_value,
    w_query,
    w_out,
    w_ret_out,
    ret_query,
    ret_key,
    ret_value,
    gate,
    decay_exp,
    mask_start,
):
    kv, queries, grad_out, lower_queries = gather_project(
        second_in, cotangent, mid, w_key, w_value, w_query, w_out
    )

    query_grad, upper = attention(mask_start, queries, grad_out, kv, None)
    upstream, grad_out, *kept = first_sum(
        decay_exp, query_grad, cotangent, gate, ret_query, ret_key, ret_value, w_query, w_out
    )
    query_grad, kv_part = attention(mask_start, lower_queries, grad_out, kv, upper)
    grad_mid, totals, grad_query, inner_key, inner_value, own_grads, grads = second_sum(
        kv_part, query_grad, upstream, mid,
        kept, ret_query, ret_key, ret_value, w_query, w_key, w_value, w_ret_out,
    )
    grad_key, grad_value, grad_w_key, grad_w_value = last(
        kept[0], kept[4], grads, own_grads, inner_key, inner_value, ret_key, ret_value, totals
    )
    return (grad_mid, grad_query, grad_key, grad_value, grad_w_key, grad_w_value)


def solution(mesh):
    placed = (
        P("seq", None),
        P("seq", None),
        P("seq", None),
        P(None, "head"),
        P(None, "head"),
        P(None, None, "head"),
        P(None, "head", None),
        P("head", None),
        P("seq", "head"),
        P("seq", "head"),
        P("seq", "head"),
        P("head", "seq"),
        P("head"),
        P("seq"),
    )
    return jax.shard_map(
        local,
        mesh=mesh,
        in_specs=placed,
        out_specs=(
            P("seq", None),
            P("seq", "head"),
            P("seq", "head"),
            P("seq", "head"),
            P(None, "head"),
            P(None, "head"),
        ),
        check_vma=False,
    )
```

```python
import functools
import math

import jax
import jax.numpy as jnp
from jax import lax
from jax.experimental import pallas as pl
from jax.experimental.pallas import tpu as pltpu
from jax.sharding import PartitionSpec as P

E = 128
BLK = 128
RC = 128
F32 = jnp.float32
BF16 = jnp.bfloat16


def contract_last(left, right):
    return lax.dot_general(left, right, (((1,), (1,)), ((), ())), preferred_element_type=F32)


def contract_first(left, right):
    return lax.dot_general(left, right, (((0,), (0,)), ((), ())), preferred_element_type=F32)


def send(src, dst, send_sem, recv_sem, axis, index):
    return pltpu.make_async_remote_copy(
        src_ref=src,
        dst_ref=dst,
        send_sem=send_sem,
        recv_sem=recv_sem,
        device_id={axis: index},
        device_id_type=pl.DeviceIdType.MESH,
    )


class SeqPlace:
    def __init__(self):
        self.peers = lax.axis_size("seq")
        self.chips = self.peers // 2
        self.me = lax.axis_index("seq")
        self.chip = self.me // 2
        self.core = lax.rem(self.me, 2)
        self.sibling = self.me + 1 - 2 * self.core

    def mate(self, k):
        return lax.rem(self.me + 2 * k, self.peers)

    def mate_of_sibling(self, k):
        return lax.rem(self.sibling + 2 * k, self.peers)


def rows_at(ref, index, rows):
    return ref.at[pl.ds(pl.multiple_of(index * rows, rows), rows)]


class Gather:
    def __init__(self, place, source, out, sems):
        self.place, self.source, self.out = place, source, out
        self.sends, self.forwards, self.arrivals = sems
        self.rows = out.shape[0] // place.peers

    @staticmethod
    def semaphores(peers):
        return [
            pltpu.SemaphoreType.DMA((peers // 2,)),
            pltpu.SemaphoreType.DMA((peers // 2,)),
            pltpu.SemaphoreType.DMA((peers,)),
        ]

    def chunk(self, index):
        return rows_at(self.out, index, self.rows)

    def direct(self, k):
        p = self.place
        return send(self.source, self.chunk(p.me), self.sends.at[k], self.arrivals.at[p.me], "seq", p.mate(k))

    def relayed(self, k):
        p = self.place
        at = p.mate(k)
        src = self.source if k == 0 else self.chunk(at)
        return send(src, self.chunk(at), self.forwards.at[k], self.arrivals.at[at], "seq", p.sibling)

    def arrival(self, index):
        p = self.place
        return send(self.source, self.chunk(index), self.sends.at[0], self.arrivals.at[index], "seq", p.sibling)

    def start(self):
        for k in range(1, self.place.chips):
            self.direct(k).start()
        self.relayed(0).start()

    def relay(self):
        for k in range(1, self.place.chips):
            self.arrival(self.place.mate(k)).wait_recv()
            self.relayed(k).start()

    def finish(self):
        p = self.place
        for k in range(p.chips):
            self.arrival(p.mate_of_sibling(k)).wait_recv()
        for k in range(1, p.chips):
            self.direct(k).wait_send()
        for k in range(p.chips):
            self.relayed(k).wait_send()


class Scatter:
    def __init__(self, place, source, scratch):
        self.place, self.source = place, source
        self.from_sibling, self.summed, self.landed = scratch[:3]
        self.pair_send, self.pair_recv, self.far_send, self.far_recv = scratch[3:]

    @staticmethod
    def scratch(peers, *chunk):
        chips = peers // 2
        return [pltpu.VMEM((chips, *chunk), BF16)] * 3 + [pltpu.SemaphoreType.DMA((chips,))] * 4

    def pair(self, i):
        p = self.place
        return send(
            self.source.at[2 * i + 1 - p.core],
            self.from_sibling.at[i],
            self.pair_send.at[i],
            self.pair_recv.at[i],
            "seq",
            p.sibling,
        )

    def far(self, k):
        p = self.place
        return send(
            self.summed.at[k], self.landed.at[k], self.far_send.at[k], self.far_recv.at[k], "seq", p.mate(k)
        )

    def pair_total(self, i):
        p = self.place
        self.pair(i).wait_recv()
        return self.source[2 * i + p.core].astype(F32) + self.from_sibling[i].astype(F32)

    def start(self):
        for k in range(self.place.chips):
            self.pair(lax.rem(self.place.chip + 1 + k, self.place.chips)).start()

    def combine(self):
        p = self.place
        for k in range(1, p.chips):
            self.summed[k] = self.pair_total(lax.rem(p.chip + k, p.chips)).astype(BF16)
            self.far(k).start()

    def total(self):
        p = self.place
        total = self.pair_total(p.chip)
        for k in range(1, p.chips):
            self.far(k).wait_recv()
            total = total + self.landed[k].astype(F32)
        return total

    def finish(self):
        for i in range(self.place.chips):
            self.pair(i).wait_send()
        for k in range(1, self.place.chips):
            self.far(k).wait_send()


SUB = 2
AHEAD = 3


class LineSum:
    def __init__(self, residual, total, scratch, produce, consume):
        self.residual, self.total = residual, total
        self.landed, self.summed = scratch[:2]
        self.in_send, self.in_recv, self.swap_recv, self.back_send, self.back_recv = scratch[2:]
        self.produce, self.consume = produce, consume
        self.count, self.rows, self.width = self.summed.shape
        self.n = lax.axis_size("head")
        self.z = lax.axis_index("head")
        low = self.z < self.n // 2
        self.depth = jnp.where(low, self.z, self.n - 1 - self.z)
        self.inward = jnp.where(low, self.z + 1, self.z - 1)
        self.outward = jnp.where(low, self.z - 1, self.z + 1)
        self.inner = self.depth == self.n // 2 - 1
        self.outer = self.depth == 0
        self.lag = self.n // 2 - self.depth + jnp.where(self.outer, AHEAD, 0)
        self.steps = self.count + self.lag

    @staticmethod
    def scratch(count, rows, width):
        sems = pltpu.SemaphoreType.DMA((count, SUB))
        return [pltpu.VMEM((count, rows, width), BF16)] * 2 + [sems] * 5

    def piece(self, j, s):
        size = self.rows // SUB
        return j, pl.ds(s * size, size)

    def up(self, j, s):
        at = self.piece(j, s)
        return send(
            self.summed.at[at], self.landed.at[at], self.in_send.at[j, s], self.in_recv.at[j, s],
            "head", self.inward,
        )

    def swap(self, j, s):
        at = self.piece(j, s)
        return send(
            self.summed.at[at], self.total.at[at], self.in_send.at[j, s], self.swap_recv.at[j, s],
            "head", self.inward,
        )

    def back(self, j, s):
        at = self.piece(j, s)
        return send(
            self.total.at[at], self.total.at[at], self.back_send.at[j, s], self.back_recv.at[j, s],
            "head", self.outward,
        )

    def reduce(self, j):
        part = self.produce(j)
        size = self.rows // SUB
        for s in range(SUB):
            at = self.piece(j, s)
            mine = part[s * size : (s + 1) * size]

            @pl.when(self.outer)
            def _(at=at, mine=mine):
                self.summed[at] = mine.astype(BF16)

            @pl.when(jnp.logical_not(self.outer))
            def _(at=at, mine=mine, s=s):
                self.up(j, s).wait_recv()
                self.summed[at] = (mine + self.landed[at].astype(F32)).astype(BF16)

            @pl.when(self.inner)
            def _(s=s):
                self.swap(j, s).start()

            @pl.when(jnp.logical_not(self.inner))
            def _(s=s):
                self.up(j, s).start()

    def finish_chunk(self, j):
        columns = pl.ds(pl.multiple_of(j * self.width, self.width), self.width)
        size = self.rows // SUB
        for s in range(SUB):
            at = self.piece(j, s)

            @pl.when(self.inner)
            def _(at=at, s=s):
                self.swap(j, s).wait_recv()
                both = self.summed[at].astype(F32) + self.total[at].astype(F32)
                if len(self.residual.shape) == 3:
                    rest = self.residual[at].astype(F32)
                else:
                    rest = self.residual[pl.ds(s * size, size), columns].astype(F32)
                self.total[at] = (rest + both).astype(BF16)

            @pl.when(jnp.logical_not(self.inner))
            def _(s=s):
                self.back(j, s).wait_recv()

            @pl.when(jnp.logical_not(self.outer))
            def _(s=s):
                self.back(j, s).start()

        self.consume(j)

    def run(self, first, last, beside=None):
        def step(t, carry):
            @pl.when(t < self.count)
            def _():
                self.reduce(t)

            @pl.when(t >= self.lag)
            def _():
                self.finish_chunk(t - self.lag)

            if beside is not None:
                beside(t)
            return carry

        lax.fori_loop(first, last, step, 0)

    def finish(self):
        def step(j, carry):
            for s in range(SUB):
                self.up(j, s).wait_send()

                @pl.when(jnp.logical_not(self.outer))
                def _(s=s):
                    self.back(j, s).wait_send()

            return carry

        lax.fori_loop(0, self.count, step, 0)


class Stream:
    def __init__(self, source, held, sem):
        self.source, self.held, self.sem = source, held, sem
        self.count = held.shape[0]

    def copy(self, i):
        return pltpu.make_async_copy(self.source(i), self.held.at[i], self.sem.at[i])

    def start(self):
        for i in range(self.count):
            self.copy(i).start()

    def wait(self, i):
        self.copy(i).wait()


def row_tiles(ref, layer, size):
    if layer is None:
        return lambda i: ref.at[pl.ds(pl.multiple_of(i * size, size), size), :]
    return lambda i: ref.at[layer, pl.ds(pl.multiple_of(i * size, size), size), :]


def column_tiles(ref, layer, size):
    if layer is None:
        return lambda i: ref.at[:, pl.ds(pl.multiple_of(i * size, size), size)]
    return lambda i: ref.at[layer, :, pl.ds(pl.multiple_of(i * size, size), size)]


def meet(seq, head):
    barrier = pltpu.get_barrier_semaphore()
    expected = 0

    def greet(axis, index):
        pl.semaphore_signal(
            barrier, inc=1, device_id={axis: index}, device_id_type=pl.DeviceIdType.MESH
        )

    if seq is not None:
        for k in range(1, seq.chips):
            greet("seq", seq.mate(k))
        greet("seq", seq.sibling)
        expected = seq.chips
    if head:
        n, z = lax.axis_size("head"), lax.axis_index("head")

        @pl.when(z > 0)
        def _():
            greet("head", z - 1)

        @pl.when(z < n - 1)
        def _():
            greet("head", z + 1)

        expected = expected + jnp.where(z > 0, 1, 0) + jnp.where(z < n - 1, 1, 0)
    pl.semaphore_wait(barrier, expected)


def call(kernel, name, number, outs, scratch, *operands, far=0, limit=56, near=0):
    whole = pl.BlockSpec(memory_space=pltpu.VMEM)
    return pl.pallas_call(
        kernel,
        out_shape=outs,
        in_specs=[pl.BlockSpec(memory_space=pltpu.SMEM)] * near
        + [whole] * (len(operands) - far - near)
        + [pl.BlockSpec(memory_space=pltpu.HBM)] * far,
        out_specs=jax.tree.map(lambda _: whole, outs),
        scratch_shapes=scratch,
        compiler_params=pltpu.CompilerParams(
            collective_id=number, has_side_effects=True, vmem_limit_bytes=limit * 2**20
        ),
        name=name,
    )(*operands)


def gather_kernel(x_ref, out_ref, *sems):
    place = SeqPlace()
    meet(place, False)
    gather = Gather(place, x_ref, out_ref, sems)
    gather.start()
    out_ref[pl.ds(pl.multiple_of(place.me * gather.rows, gather.rows), gather.rows), :] = x_ref[...]
    gather.relay()
    gather.finish()


def gather_seq(x, name, number):
    peers = lax.axis_size("seq")
    out = jax.ShapeDtypeStruct((peers * x.shape[0], x.shape[1]), x.dtype)
    return call(gather_kernel, name, number, out, Gather.semaphores(peers), x)


def tile_of(width):
    return 256 if width % 256 == 0 else E


def gather_project_kernel(
    second_far, cotangent_far, mid_far, wk_ref, wv_ref, wq_ref, wo_ref,
    out_ref, q1_ref, g1_ref, q0_ref,
    second_ref, cotangent_ref, mid_ref, kv_columns, columns, rows,
    input_sem, kv_sem, column_sem, row_sem, *sems
):
    place = SeqPlace()
    width = q1_ref.shape[1]
    tile = tile_of(width)
    pieces = width // tile
    half = out_ref.shape[1] // 2

    def kv_copy(i):
        return pltpu.make_async_copy((wk_ref, wv_ref)[i], kv_columns.at[i], kv_sem.at[i])

    def column_copy(layer, i):
        return pltpu.make_async_copy(
            wq_ref.at[layer, :, pl.ds(i * tile, tile)], columns.at[layer, i], column_sem.at[layer, i]
        )

    def row_copy(i):
        return pltpu.make_async_copy(wo_ref.at[1, pl.ds(i * tile, tile), :], rows.at[i], row_sem.at[i])

    def input_copy(i):
        source = (mid_far, second_far, cotangent_far)[i]
        return pltpu.make_async_copy(source, (mid_ref, second_ref, cotangent_ref)[i], input_sem.at[i])

    input_copy(0).start()
    for i in range(2):
        kv_copy(i).start()
    input_copy(1).start()
    for i in range(pieces):
        column_copy(1, i).start()
    input_copy(2).start()
    for i in range(pieces):
        row_copy(i).start()
    for i in range(pieces):
        column_copy(0, i).start()
    own = rows_at(out_ref, place.me, out_ref.shape[0] // place.peers)
    gather = Gather(place, own, out_ref, sems)
    input_copy(0).wait()
    for i in range(2):
        kv_copy(i).wait()
        own[:, i * half : (i + 1) * half] = jnp.dot(
            mid_ref[...], kv_columns[i], preferred_element_type=F32
        ).astype(BF16)
    meet(place, False)
    gather.start()
    input_copy(1).wait()
    for i in range(pieces):
        column_copy(1, i).wait()
        q1_ref[:, i * tile : (i + 1) * tile] = jnp.dot(
            second_ref[...], columns[1, i], preferred_element_type=F32
        ).astype(BF16)
    input_copy(2).wait()
    for i in range(pieces):
        row_copy(i).wait()
        g1_ref[:, i * tile : (i + 1) * tile] = contract_last(cotangent_ref[...], rows[i]).astype(BF16)
    for i in range(pieces):
        column_copy(0, i).wait()
        q0_ref[:, i * tile : (i + 1) * tile] = jnp.dot(
            mid_ref[...], columns[0, i], preferred_element_type=F32
        ).astype(BF16)
    gather.relay()
    gather.finish()


def gather_project(second_in, cotangent, mid, w_key, w_value, w_query, w_out):
    peers = lax.axis_size("seq")
    depth, width = w_query.shape[1:]
    tile = tile_of(width)
    pieces = width // tile
    half = w_key.shape[1]
    projected = jax.ShapeDtypeStruct((mid.shape[0], width), BF16)
    outs = (jax.ShapeDtypeStruct((peers * mid.shape[0], 2 * half), BF16),) + (projected,) * 3
    scratch = [
        pltpu.VMEM(second_in.shape, BF16),
        pltpu.VMEM(cotangent.shape, BF16),
        pltpu.VMEM(mid.shape, BF16),
        pltpu.VMEM((2, depth, half), BF16),
        pltpu.VMEM((2, pieces, depth, tile), BF16),
        pltpu.VMEM((pieces, tile, depth), BF16),
        pltpu.SemaphoreType.DMA((3,)),
        pltpu.SemaphoreType.DMA((2,)),
        pltpu.SemaphoreType.DMA((2, pieces)),
        pltpu.SemaphoreType.DMA((pieces,)),
    ] + Gather.semaphores(peers)
    return call(
        gather_project_kernel, "gather_kv", 0, outs, scratch,
        second_in, cotangent, mid, w_key, w_value, w_query, w_out, far=7, limit=52,
    )


class Retention:
    def __init__(self, decay):
        self.decay = decay
        self.count = decay.shape[1]

    def columns(self, h):
        return pl.ds(pl.multiple_of(h * E, E), E)

    def tile(self, ref, h, c):
        return ref[c * RC : (c + 1) * RC, self.columns(h)]

    def row(self, h, c):
        return self.decay[h, c : c + 1, :]

    def across(self, h, c):
        row = jnp.broadcast_to(self.row(h, c), (RC, RC))
        return row, jnp.transpose(row)

    def end(self, h, c):
        return self.row(h, c)[:, RC - 1 : RC]

    def weights(self, row, column):
        later = lax.broadcasted_iota(jnp.int32, (RC, RC), 0)
        lower = later >= lax.broadcasted_iota(jnp.int32, (RC, RC), 1)
        return jnp.where(lower, jnp.exp(jnp.where(lower, column - row, 0.0)), 0.0)


def running_sum(values):
    lane = lax.rem(lax.broadcasted_iota(jnp.int32, values.shape, 1), RC)
    shift = 1
    while shift < RC:
        values = values + jnp.where(lane >= shift, pltpu.roll(values, shift, 1), 0.0)
        shift *= 2
    return values


def first_sum_kernel(
    exponent, query_grad, residual, gate, ret_query, ret_key, ret_value, wq_ref, wo_ref,
    total, grad_out, accum, second, own_states, states, decays,
    logs, wq, wo, acc, wq_sem, wo_sem, *scratch
):
    place = SeqPlace()
    width = wq.shape[1]
    heads = second.shape[0]
    wq_tiles = Stream(row_tiles(wq_ref, 1, width), wq, wq_sem)
    wo_tiles = Stream(column_tiles(wo_ref, 0, width), wo, wo_sem)
    wq_tiles.start()
    wo_tiles.start()

    def produce(j):
        wq_tiles.wait(j)
        return contract_last(query_grad[...], wq[j])

    def consume(j):
        wo_tiles.wait(j)
        acc[...] += contract_last(total[j], wo[j])

    meet(place, True)
    line = LineSum(residual, total, scratch[:7], produce, consume)
    own_decay = rows_at(decays, place.me, decays.shape[0] // place.peers)
    own_state = rows_at(states, place.me, states.shape[0] // place.peers)
    small = Gather(place, own_decay, decays, scratch[7:10])
    large = Gather(place, own_state, states, scratch[10:13])
    acc[...] = jnp.zeros_like(acc)
    for h in range(heads):
        power = jnp.broadcast_to(-exponent[h].astype(F32) / 64.0, (1, gate.shape[1]))
        logs[h : h + 1, :] = -jnp.exp2(power) * gate[h : h + 1, :]
    sums = running_sum(logs[...])
    for h in range(heads):
        for c in range(accum.shape[1]):
            accum[h, c : c + 1, :] = sums[h : h + 1, c * RC : (c + 1) * RC]
    own_decay[...] = jnp.zeros_like(own_decay)
    ret = Retention(accum)

    def beside(h):
        @pl.when(h < heads)
        def _():
            state = jnp.zeros((E, E), F32)
            decay = jnp.zeros((1, 1), F32)
            for c in range(ret.count):
                row, column = ret.across(h, c)
                end = ret.end(h, c)
                key = ret.tile(ret_key, h, c)
                shrunk = (jnp.exp(end - column) * key.astype(F32)).astype(BF16)
                here = contract_first(shrunk, ret.tile(ret_value, h, c))
                own_states[h, c] = here
                state = jnp.exp(end) * state + here
                decay = decay + end
                products = contract_last(ret.tile(ret_query, h, c), key)
                second[h, c] = (ret.weights(row, column) * products).astype(BF16)
            states[pl.ds(pl.multiple_of((place.me * heads + h) * E, E), E), :] = state.astype(BF16)
            decays[pl.ds(place.me * own_decay.shape[0] + h, 1), :] = jnp.broadcast_to(decay, (1, E))

    line.run(0, heads, beside)
    small.start()
    large.start()
    line.run(heads, line.steps - 1)
    small.relay()
    large.relay()
    line.run(line.steps - 1, line.steps)
    grad_out[...] = acc[...].astype(BF16)
    small.finish()
    large.finish()
    line.finish()


def first_sum(decay_exp, query_grad, residual, gate, ret_query, ret_key, ret_value, w_query, w_out):
    peers = lax.axis_size("seq")
    rows, depth = residual.shape
    heads_width = query_grad.shape[1]
    out_width = w_out.shape[1]
    width = tile_of(depth)
    count = depth // width
    heads = ret_query.shape[1] // E
    blocks = rows // RC
    group = heads + -heads % 8
    outs = (
        jax.ShapeDtypeStruct((count, rows, width), BF16),
        jax.ShapeDtypeStruct((rows, out_width), BF16),
        jax.ShapeDtypeStruct((heads, blocks, RC), F32),
        jax.ShapeDtypeStruct((heads, blocks, RC, RC), BF16),
        jax.ShapeDtypeStruct((heads, blocks, E, E), F32),
        jax.ShapeDtypeStruct((peers * heads * E, E), BF16),
        jax.ShapeDtypeStruct((peers * group, E), F32),
    )
    scratch = [
        pltpu.VMEM((group, rows), F32),
        pltpu.VMEM((count, width, heads_width), BF16),
        pltpu.VMEM((count, out_width, width), BF16),
        pltpu.VMEM((rows, out_width), F32),
        pltpu.SemaphoreType.DMA((count,)),
        pltpu.SemaphoreType.DMA((count,)),
    ] + LineSum.scratch(count, rows, width) + Gather.semaphores(peers) + Gather.semaphores(peers)
    return call(
        first_sum_kernel, "first_sum", 1, outs, scratch,
        decay_exp, query_grad, residual, gate, ret_query, ret_key, ret_value, w_query, w_out,
        far=2, limit=22, near=1,
    )


def second_sum_kernel(
    kv_part, query_grad, residual, mid,
    accum, second, own_states, states, decays, ret_query, ret_key, ret_value,
    wq_ref, wk_ref, wv_ref, wo_ref,
    grad_mid, totals, grad_query, inner_key, inner_value, own_grads, grads,
    grad_o, entering, total, wq, wk, wv, wo, part, kv_grad, weights, acc,
    wq_sem, wk_sem, wv_sem, wo_sem, *scratch
):
    place = SeqPlace()
    count, rows, width = part.shape
    half = kv_grad.shape[1] // 2
    wq_tiles = Stream(row_tiles(wq_ref, 0, width), wq, wq_sem)
    wk_tiles = Stream(row_tiles(wk_ref, None, width), wk, wk_sem)
    wv_tiles = Stream(row_tiles(wv_ref, None, width), wv, wv_sem)
    wo_tiles = Stream(column_tiles(wo_ref, None, width), wo, wo_sem)
    for tiles in (wq_tiles, wk_tiles, wv_tiles, wo_tiles):
        tiles.start()

    def produce(j):
        wk_tiles.wait(j)
        wv_tiles.wait(j)
        return (
            part[j]
            + contract_last(kv_grad[:, :half], wk[j])
            + contract_last(kv_grad[:, half:], wv[j])
        )

    def consume(j):
        wo_tiles.wait(j)
        acc[...] += contract_last(total[j], wo[j])

    def lower(j, carry):
        wq_tiles.wait(j)
        part[j] = contract_last(query_grad[...], wq[j])
        return carry

    meet(place, True)
    scatter_kv = Scatter(place, kv_part, scratch[7:14])
    scatter_kv.start()
    lax.fori_loop(0, 2, lower, 0)
    scatter_kv.combine()
    lax.fori_loop(2, count, lower, 0)
    acc[...] = jnp.zeros_like(acc)
    across = scatter_kv.total()
    for side in (0, 1):
        kv_grad[:, side * half : (side + 1) * half] = jnp.transpose(across[side]).astype(BF16)
    line = LineSum(residual, total, scratch[:7], produce, consume)
    scatter = Scatter(place, weights, scratch[14:21])
    own = rows_at(totals, place.me, totals.shape[0] // place.peers)
    gather = Gather(place, own, totals, scratch[21:24])
    ends = Gather(place, rows_at(grads, place.me, grads.shape[0] // place.peers), grads, scratch[24:27])
    ret = Retention(accum)
    heads = second.shape[0]
    group = decays.shape[0] // place.peers

    def beside(t):
        h = t - late

        @pl.when((h >= 0) & (h < heads))
        def _():
            def hop(s, state):
                grown = jnp.exp(decays[pl.ds(s * group + h, 1), :]) * state
                return grown + states[pl.ds(pl.multiple_of((s * heads + h) * E, E), E), :].astype(F32)

            state = lax.fori_loop(0, place.me, hop, jnp.zeros((E, E), F32))
            for c in range(ret.count):
                entering[h, c] = state.astype(BF16)
                state = jnp.exp(ret.end(h, c)) * state + own_states[h, c]

    def own_grad(h, carry):
        state = jnp.zeros((E, E), F32)
        for c in reversed(range(ret.count)):
            row, column = ret.across(h, c)
            grown = (jnp.exp(column) * ret.tile(ret_query, h, c).astype(F32)).astype(BF16)
            here = contract_first(grown, ret.tile(grad_o, h, c)) * (1.0 / E)
            own_grads[h, c] = here
            state = here + jnp.exp(ret.end(h, c)) * state
        grads[pl.ds(pl.multiple_of((place.me * heads + h) * E, E), E), :] = state.astype(BF16)
        return carry

    def inner(h, carry):
        for c in range(ret.count):
            row, column = ret.across(h, c)
            rows_here = slice(c * RC, (c + 1) * RC)
            grad = ret.tile(grad_o, h, c)
            products = contract_last(grad, ret.tile(ret_value, h, c))
            first = (ret.weights(row, column) * products).astype(BF16)
            near = jnp.dot(first, ret.tile(ret_key, h, c), preferred_element_type=F32)
            carried = contract_last(grad, entering[h, c])
            grad_query[rows_here, ret.columns(h)] = (
                (near + jnp.exp(column) * carried) * (1.0 / E)
            ).astype(BF16)
            inner_key[rows_here, ret.columns(h)] = contract_first(first, ret.tile(ret_query, h, c)) * (1.0 / E)
            inner_value[rows_here, ret.columns(h)] = contract_first(second[h, c], grad) * (1.0 / E)
        return carry

    early = line.lag - 1
    late = line.steps - 1 - heads
    line.run(0, early)
    size = weights.shape[1]
    for i in range(place.peers):
        weights[i] = contract_first(mid[:, i * size : (i + 1) * size], kv_grad[...]).astype(BF16)
    scatter.start()
    line.run(early, early + 2)
    scatter.combine()
    line.run(early + 2, early + 9, beside)
    own[...] = scatter.total().astype(BF16)
    gather.start()
    line.run(early + 9, line.steps, beside)
    grad_o[...] = acc[...].astype(BF16)
    lax.fori_loop(0, heads, own_grad, 0)
    ends.start()
    for j in range(count):
        grad_mid[:, j * width : (j + 1) * width] = total[j]
    gather.relay()
    lax.fori_loop(0, heads, inner, 0)
    gather.finish()
    scatter.finish()
    ends.relay()
    ends.finish()
    scatter_kv.finish()
    line.finish()


def second_sum(kv_part, query_grad, residual, mid, kept, ret_query, ret_key, ret_value, w_query, w_key, w_value, w_ret_out):
    peers = lax.axis_size("seq")
    rows, depth = mid.shape
    heads_width = query_grad.shape[1]
    out_width = w_ret_out.shape[0]
    both = 2 * w_key.shape[1]
    width = tile_of(depth)
    count = depth // width
    outs = (
        jax.ShapeDtypeStruct((rows, depth), BF16),
        jax.ShapeDtypeStruct((depth, both), BF16),
        jax.ShapeDtypeStruct((rows, out_width), BF16),
        jax.ShapeDtypeStruct((rows, out_width), F32),
        jax.ShapeDtypeStruct((rows, out_width), F32),
        jax.ShapeDtypeStruct(kept[2].shape, F32),
        jax.ShapeDtypeStruct(kept[3].shape, BF16),
    )
    scratch = [
        pltpu.VMEM((rows, out_width), BF16),
        pltpu.VMEM(kept[2].shape, BF16),
        pltpu.VMEM((count, rows, width), BF16),
        pltpu.VMEM((count, width, heads_width), BF16),
        pltpu.VMEM((count, width, both // 2), BF16),
        pltpu.VMEM((count, width, both // 2), BF16),
        pltpu.VMEM((count, out_width, width), BF16),
        pltpu.VMEM((count, rows, width), F32),
        pltpu.VMEM((rows, both), BF16),
        pltpu.VMEM((peers, depth // peers, both), BF16),
        pltpu.VMEM((rows, out_width), F32),
    ] + [pltpu.SemaphoreType.DMA((count,))] * 4
    scratch += (
        LineSum.scratch(count, rows, width)
        + Scatter.scratch(peers, *kv_part.shape[1:])
        + Scatter.scratch(peers, depth // peers, both)
        + Gather.semaphores(peers)
        + Gather.semaphores(peers)
    )
    return call(
        second_sum_kernel, "second_sum", 3, outs, scratch,
        kv_part, query_grad, residual, mid, *kept, ret_query, ret_key, ret_value,
        w_query, w_key, w_value, w_ret_out, far=4, limit=39,
    )


def last_kernel(
    accum, decays, grads, own_grads, inner_key, inner_value, ret_key, ret_value, totals,
    grad_key, grad_value, grad_w_key, grad_w_value, wide, sems
):
    place = SeqPlace()
    ret = Retention(accum)
    heads = own_grads.shape[0]
    group = decays.shape[0] // place.peers
    pieces, size, half = wide.shape[1:]

    def copy(side, i):
        out = (grad_w_key, grad_w_value)[side]
        return pltpu.make_async_copy(wide.at[side, i], out.at[pl.ds(i * size, size)], sems.at[side, i])

    for i in range(pieces):
        for side in (0, 1):
            wide[side, i] = totals[i * size : (i + 1) * size, side * half : (side + 1) * half].astype(F32)
            copy(side, i).start()

    def head(h, carry):
        def hop(k, state):
            s = place.peers - 1 - k
            here = grads[pl.ds(pl.multiple_of((s * heads + h) * E, E), E), :].astype(F32)
            return here + jnp.exp(decays[pl.ds(s * group + h, 1), :]) * state

        state = lax.fori_loop(0, place.peers - 1 - place.me, hop, jnp.zeros((E, E), F32))
        for c in reversed(range(ret.count)):
            rows_here = slice(c * RC, (c + 1) * RC)
            row, column = ret.across(h, c)
            end = ret.end(h, c)
            after = state.astype(BF16)
            shrink = jnp.exp(end - column)
            at_key = contract_last(ret.tile(ret_value, h, c), after)
            at_value = jnp.dot(ret.tile(ret_key, h, c), after, preferred_element_type=F32)
            grad_key[rows_here, ret.columns(h)] = (
                inner_key[rows_here, ret.columns(h)] + shrink * at_key
            ).astype(BF16)
            grad_value[rows_here, ret.columns(h)] = (
                inner_value[rows_here, ret.columns(h)] + shrink * at_value
            ).astype(BF16)
            state = own_grads[h, c] + jnp.exp(end) * state
        return carry

    lax.fori_loop(0, heads, head, 0)
    for i in range(pieces):
        for side in (0, 1):
            copy(side, i).wait()


def last(accum, decays, grads, own_grads, inner_key, inner_value, ret_key, ret_value, totals):
    depth, both = totals.shape
    pieces = 6 if depth % (6 * E) == 0 else 1
    whole = pl.BlockSpec(memory_space=pltpu.VMEM)
    far = pl.BlockSpec(memory_space=pltpu.HBM)
    wide = jax.ShapeDtypeStruct((depth, both // 2), F32)
    narrow = jax.ShapeDtypeStruct(ret_key.shape, BF16)
    return pl.pallas_call(
        last_kernel,
        out_shape=(narrow, narrow, wide, wide),
        in_specs=[whole] * 9,
        out_specs=(whole, whole, far, far),
        scratch_shapes=[
            pltpu.VMEM((2, pieces, depth // pieces, both // 2), F32),
            pltpu.SemaphoreType.DMA((2, pieces)),
        ],
        compiler_params=pltpu.CompilerParams(vmem_limit_bytes=24 * 2**20),
        name="last",
    )(accum, decays, grads, own_grads, inner_key, inner_value, ret_key, ret_value, totals)


UNROLL = (4, 2, 1)


def sweep(first, last, body, carry):
    for width in UNROLL:
        many = jnp.maximum(last - first, 0) // width

        def several(i, carry, first=first, width=width):
            for k in range(width):
                carry = body(first + width * i + k, carry)
            return carry

        carry = lax.fori_loop(0, many, several, carry)
        first = first + width * many
    return carry


def attention_kernel(group, has_prev, mask_ref, *refs):
    if has_prev:
        q_all, g_all, kv_ref, prev_ref, dq_all, dkv_ref, s_ref, acc_all = refs
        acc_all[...] = prev_ref[...]
    else:
        q_all, g_all, kv_ref, dq_all, dkv_ref, s_ref = refs
        acc_all = dkv_ref
        acc_all[...] = jnp.zeros_like(acc_all)
    heads = acc_all.shape[2] // E
    blocks = q_all.shape[0] // BLK

    def tile(i, carry):
        h, b = i // blocks, lax.rem(i, blocks)
        at = pl.ds(pl.multiple_of(b * BLK, BLK), BLK)
        across = pl.ds(pl.multiple_of(h * group * E, E), group * E)
        here = pl.ds(pl.multiple_of(h * E, E), E)
        attention_tile(
            group, mask_ref, b, q_all.at[at, across], g_all.at[at, across], kv_ref.at[:, here],
            kv_ref.at[:, pl.ds(pl.multiple_of((heads + h) * E, E), E)],
            dq_all.at[at, across], acc_all.at[:, :, here], s_ref,
        )
        return carry

    lax.fori_loop(0, heads * blocks, tile, 0)
    if has_prev:
        dkv_ref[...] = acc_all[...].astype(BF16)


def attention_tile(group, mask_ref, block, q_ref, g_ref, k_ref, v_ref, dq_ref, acc, s_ref):
    step = acc.shape[3]
    factor = 1.0 / math.sqrt(E)
    power = factor * math.log2(math.e)
    first_row = lax.axis_index("seq") * step + block * BLK
    first_key = mask_ref[block]
    rows = group * BLK
    q = jnp.concatenate([q_ref[:, i * E : (i + 1) * E] for i in range(group)], axis=0)
    g = jnp.concatenate([g_ref[:, i * E : (i + 1) * E] for i in range(group)], axis=0)
    q_across, g_across = jnp.transpose(q), jnp.transpose(g)
    low = first_key // step
    high = (first_row + BLK + step - 1) // step

    def span(j):
        return pl.ds(pl.multiple_of(j * step, step), step)

    def fold(values, combine):
        total = values[:, :E]
        for i in range(1, step // E):
            total = combine(total, values[:, i * E : (i + 1) * E])
        return total

    def score(masked, j, top):
        scores = contract_last(q, k_ref[span(j), :])
        if masked:
            at = j * step + lax.broadcasted_iota(jnp.int32, (BLK, step), 1)
            query_position = first_row + lax.broadcasted_iota(jnp.int32, (BLK, step), 0)
            seen = (at >= first_key) & (at <= query_position)
            seen = jnp.concatenate([seen] * group, axis=0)
            scores = jnp.where(seen, scores, -jnp.inf)
        s_ref[:, span(j)] = scores
        return jnp.maximum(top, fold(scores, jnp.maximum))

    inside, outside = functools.partial(score, False), functools.partial(score, True)
    top = outside(low, jnp.full((rows, E), -jnp.inf, F32))
    top = sweep(low + 1, high - 1, inside, top)
    top = lax.fori_loop(jnp.maximum(low + 1, high - 1), high, outside, top)
    top = jnp.max(top, axis=-1, keepdims=True)

    def raise_(j, total):
        raised = jnp.exp2((s_ref[:, span(j)] - top) * power)
        s_ref[:, span(j)] = raised
        return total + fold(raised, jnp.add)

    total = sweep(low, high, raise_, jnp.zeros((rows, E), F32))
    scale = 1.0 / jnp.sum(total, axis=-1, keepdims=True)

    def output(j, out):
        probs = (s_ref[:, span(j)] * scale).astype(BF16)
        return out + jnp.dot(probs, v_ref[span(j), :], preferred_element_type=F32)

    out = sweep(low, high, output, jnp.zeros((rows, E), F32)).astype(BF16)
    delta = jnp.sum(g.astype(F32) * out.astype(F32), axis=-1, keepdims=True)

    def back(j, dq):
        probs = s_ref[:, span(j)] * scale
        dprobs = contract_last(g, v_ref[span(j), :])
        dscores = (probs * (dprobs - delta) * factor).astype(BF16)
        acc[j, 0] += jnp.dot(q_across, dscores, preferred_element_type=F32)
        acc[j, 1] += jnp.dot(g_across, probs.astype(BF16), preferred_element_type=F32)
        return dq + jnp.dot(dscores, k_ref[span(j), :], preferred_element_type=F32)

    dq = sweep(low, high, back, jnp.zeros((rows, E), F32)).astype(BF16)
    for i in range(group):
        dq_ref[:, i * E : (i + 1) * E] = dq[i * BLK : (i + 1) * BLK, :]


def attention(mask_start, queries, grad_out, kv, previous):
    row_count, width = queries.shape
    key_count, both = kv.shape
    heads = both // (2 * E)
    group = width // (heads * E)
    step = row_count
    count = key_count // step
    has_prev = previous is not None
    part = jax.ShapeDtypeStruct((count, 2, heads * E, step), BF16 if has_prev else F32)
    scratch = [pltpu.VMEM((group * BLK, key_count), F32)]
    if has_prev:
        scratch += [pltpu.VMEM(part.shape, F32)]
    whole = pl.BlockSpec(memory_space=pltpu.VMEM)
    return pl.pallas_call(
        functools.partial(attention_kernel, group, has_prev),
        out_shape=(jax.ShapeDtypeStruct((row_count, width), BF16), part),
        in_specs=[pl.BlockSpec(memory_space=pltpu.SMEM)] + [whole] * (4 if has_prev else 3),
        out_specs=(whole, whole),
        scratch_shapes=scratch,
        compiler_params=pltpu.CompilerParams(vmem_limit_bytes=12 * 2**20),
        cost_estimate=pl.CostEstimate(
            flops=10 * row_count * width * key_count, bytes_accessed=8 * 2**20, transcendentals=0
        ),
        name="attention_back",
    )(mask_start, queries, grad_out, kv, *(() if previous is None else (previous,)))


def local(
    mid,
    second_in,
    cotangent,
    w_key,
    w_value,
    w_query,
    w_out,
    w_ret_out,
    ret_query,
    ret_key,
    ret_value,
    gate,
    decay_exp,
    mask_start,
):
    kv, queries, grad_out, lower_queries = gather_project(
        second_in, cotangent, mid, w_key, w_value, w_query, w_out
    )

    query_grad, upper = attention(mask_start, queries, grad_out, kv, None)
    upstream, grad_out, *kept = first_sum(
        decay_exp, query_grad, cotangent, gate, ret_query, ret_key, ret_value, w_query, w_out
    )
    query_grad, kv_part = attention(mask_start, lower_queries, grad_out, kv, upper)
    grad_mid, totals, grad_query, inner_key, inner_value, own_grads, grads = second_sum(
        kv_part, query_grad, upstream, mid,
        kept, ret_query, ret_key, ret_value, w_query, w_key, w_value, w_ret_out,
    )
    grad_key, grad_value, grad_w_key, grad_w_value = last(
        kept[0], kept[4], grads, own_grads, inner_key, inner_value, ret_key, ret_value, totals
    )
    return (grad_mid, grad_query, grad_key, grad_value, grad_w_key, grad_w_value)


def solution(mesh):
    placed = (
        P("seq", None),
        P("seq", None),
        P("seq", None),
        P(None, "head"),
        P(None, "head"),
        P(None, None, "head"),
        P(None, "head", None),
        P("head", None),
        P("seq", "head"),
        P("seq", "head"),
        P("seq", "head"),
        P("head", "seq"),
        P("head"),
        P("seq"),
    )
    return jax.shard_map(
        local,
        mesh=mesh,
        in_specs=placed,
        out_specs=(
            P("seq", None),
            P("seq", "head"),
            P("seq", "head"),
            P("seq", "head"),
            P(None, "head"),
            P(None, "head"),
        ),
        check_vma=False,
    )
```
